8 devices in a mesh: dp: 2 (over z, y), ep: 4 (over x, core).
Axes of the slice: x: 2, y: 2, z: 1, core: 2. Of those that a mesh axis runs over, the one named last changes fastest.
Arguments:
- x_in: bfloat16 [1536, 2560], P(('dp', 'ep')), parts along dimension 0
- norm_gain: bfloat16 [2560], replicated
- w_router: bfloat16 [2560, 64], replicated
- expert_ids: int32 [1536, 6], P(('dp', 'ep')), parts along dimension 0
- w_gate: bfloat16 [64, 2560, 1536], P('ep')
- w_up: bfloat16 [64, 2560, 1536], P('ep')
- w_down: bfloat16 [64, 1536, 2560], P('ep')
Outputs:
- output: bfloat16 [1536, 2560], P(('dp', 'ep')), parts along dimension 0
There are 2 independent parts. The reference program is written for one: setup_inputs(seed, part) draws one part's arguments, and reference() takes and returns one part's arrays. A program takes and returns all parts, laid end to end along the dimension named above; an argument that names none is the same for every part.
All inputs are finite; a program needn't handle non-finite values.
Results may differ from the reference program's by a relative error of at most 0.001.
Values are sent between devices in bfloat16 or wider.
A program may use at most 1.5 GiB of HBM per device.

```python
import jax
import jax.numpy as jnp
from jax import lax

HIDDEN = 2560
EXPERT_FF = 1536
EXPERTS = 64
TOP_K = 6
TOKENS = 192
GROUP_SIZE = 4

EPS = 1e-6
CAP_DEV = 2 * TOKENS * TOP_K // EXPERTS
HOT_COUNT = EXPERTS // 4
COLD_LEFT = TOKENS * TOP_K - HOT_COUNT * CAP_DEV
COLD_BASE = COLD_LEFT // (EXPERTS - HOT_COUNT)
COLD_EXTRA = COLD_LEFT % (EXPERTS - HOT_COUNT)
ROW_LIMIT = GROUP_SIZE * CAP_DEV


def draw_device(hot_flag, key):
    key_rank, key_rows, key_cols = jax.random.split(key, 3)
    expert_range = jnp.arange(EXPERTS, dtype=jnp.int32)
    noise = jax.random.randint(key_rank, (EXPERTS,), 0, EXPERTS, dtype=jnp.int32)
    score = (1 - hot_flag) * (EXPERTS * EXPERTS) + noise * EXPERTS + expert_range
    rank = jnp.argsort(jnp.argsort(score))
    counts = jnp.where(rank < HOT_COUNT, CAP_DEV, COLD_BASE + (rank - HOT_COUNT < COLD_EXTRA).astype(jnp.int32))
    bounds = jnp.cumsum(counts).astype(jnp.int32)
    flat_ids = jnp.searchsorted(bounds, jnp.arange(TOKENS * TOP_K, dtype=jnp.int32), side="right").astype(jnp.int32)
    table = flat_ids.reshape(TOP_K, TOKENS).T
    table = jax.random.permutation(key_rows, table, axis=0)
    col_score = jax.random.randint(key_cols, (TOKENS, TOP_K), 0, TOP_K, dtype=jnp.int32) * TOP_K + jnp.arange(TOP_K, dtype=jnp.int32)
    col_order = jnp.argsort(col_score, axis=1)
    return jnp.take_along_axis(table, col_order, axis=1)


def draw_routes(key):
    key_hot, key_dev = jax.random.split(key)
    hot_order = jax.random.permutation(key_hot, EXPERTS)
    hot_flag = (jnp.argsort(hot_order) < HOT_COUNT).astype(jnp.int32)
    dev_keys = jax.random.split(key_dev, GROUP_SIZE)
    routes = jax.vmap(draw_device, in_axes=(None, 0))(hot_flag, dev_keys)
    return routes.reshape(GROUP_SIZE * TOKENS, TOP_K).astype(jnp.int32)


def setup_inputs(seed: int = 0, part: int = 0) -> dict:
    shared = jax.random.split(jax.random.key(seed), 5)
    own = jax.random.split(jax.random.fold_in(jax.random.key(seed + 1), part), 2)
    x_in = (0.5 * jax.random.normal(own[0], (GROUP_SIZE * TOKENS, HIDDEN), jnp.float32)).astype(jnp.bfloat16)
    norm_gain = jax.random.uniform(shared[0], (HIDDEN,), jnp.float32, 0.5, 1.5).astype(jnp.bfloat16)
    w_router = (2.0 * HIDDEN ** -0.5 * jax.random.normal(shared[1], (HIDDEN, EXPERTS), jnp.float32)).astype(jnp.bfloat16)
    w_gate = (HIDDEN ** -0.5 * jax.random.normal(shared[2], (EXPERTS, HIDDEN, EXPERT_FF), jnp.float32)).astype(jnp.bfloat16)
    w_up = (HIDDEN ** -0.5 * jax.random.normal(shared[3], (EXPERTS, HIDDEN, EXPERT_FF), jnp.float32)).astype(jnp.bfloat16)
    w_down = (1.5 * EXPERT_FF ** -0.5 * jax.random.normal(shared[4], (EXPERTS, EXPERT_FF, HIDDEN), jnp.float32)).astype(jnp.bfloat16)
    expert_ids = draw_routes(own[1])
    return {"x_in": x_in, "norm_gain": norm_gain, "w_router": w_router, "expert_ids": expert_ids, "w_gate": w_gate, "w_up": w_up, "w_down": w_down}


def reference(x_in, norm_gain, w_router, expert_ids, w_gate, w_up, w_down):
    resid = x_in.astype(jnp.float32)
    mean_sq = jnp.mean(resid * resid, axis=-1, keepdims=True)
    normed = (resid * lax.rsqrt(mean_sq + EPS) * norm_gain.astype(jnp.float32)).astype(jnp.bfloat16)
    logits = jnp.dot(normed, w_router, preferred_element_type=jnp.float32)
    router_p = jax.nn.softmax(logits, axis=-1)
    picked = jnp.take_along_axis(router_p, expert_ids, axis=1)
    gates = picked / jnp.sum(picked, axis=1, keepdims=True)
    total = x_in.shape[0]

    def one_expert(moe_sum, inputs):
        expert, gate_w, up_w, down_w = inputs
        hits = expert_ids == expert
        weight = jnp.sum(jnp.where(hits, gates, 0.0), axis=1)
        rows = jnp.nonzero(jnp.any(hits, axis=1), size=ROW_LIMIT, fill_value=total)[0]
        sel_rows = jnp.take(normed, rows, axis=0, mode="fill", fill_value=0)
        gate_val = jnp.dot(sel_rows, gate_w, preferred_element_type=jnp.float32)
        up_val = jnp.dot(sel_rows, up_w, preferred_element_type=jnp.float32)
        hidden_act = (jax.nn.silu(gate_val) * up_val).astype(jnp.bfloat16)
        out_rows = jnp.dot(hidden_act, down_w, preferred_element_type=jnp.float32).astype(jnp.bfloat16)
        row_w = jnp.take(weight, rows, mode="fill", fill_value=0)
        moe_sum = moe_sum.at[rows].add(out_rows.astype(jnp.float32) * row_w[:, None], mode="drop")
        return moe_sum, None

    start_sum = jnp.zeros((total, HIDDEN), jnp.float32)
    moe_sum = lax.scan(one_expert, start_sum, (jnp.arange(EXPERTS, dtype=jnp.int32), w_gate, w_up, w_down))[0]
    return (resid + moe_sum).astype(jnp.bfloat16)
```

```python
import functools

import jax
import jax.numpy as jnp
from jax import lax
from jax.experimental import pallas as pl
from jax.experimental.pallas import tpu as pltpu
from jax.sharding import PartitionSpec as P

EPS = 1e-6
TOK = 192
PAD = 256
CAP = 36
CROW = 2 * CAP
EROW = 4 * CAP
NE = 16
GE = 4
KC = 512
NK = 5
FF = 1536
NF = 3
NSLOT = 16
AHEAD = NSLOT // 2
P1 = NE * NK
P2 = NK * NE // 2
SLOTS = NE * CROW
f32, bf16, i32 = jnp.float32, jnp.bfloat16, jnp.int32


def kernel(x_hbm, gain_hbm, wr_hbm, ids_hbm, wg_hbm, wu_hbm, wd_hbm, out_ref,
           xv, gv, wrv, idv, h_all, info_own, info_all, gat, cmb, acc, act, ring, xg, yb, sib, rem,
           in_sem, ring_sem, h_send, h_recv, i_send, i_recv, s_send, s_recv, r_send, r_recv):
    me = lax.axis_index("ep")
    chip = me // 2
    core = me % 2
    sibling = chip * 2 + (1 - core)
    partner = (1 - chip) * 2 + core
    diag = (1 - chip) * 2 + (1 - core)

    ins = [pltpu.make_async_copy(s, d, in_sem.at[i]) for i, (s, d) in enumerate(
        ((x_hbm, xv), (gain_hbm, gv), (wr_hbm, wrv), (ids_hbm, idv)))]
    for c in ins:
        c.start()

    def start_p1(s):
        g = s // (NK * GE)
        k = (s % (NK * GE)) // GE
        e = g * GE + s % GE
        for m, w in enumerate((wg_hbm, wu_hbm)):
            slot = (2 * s + m) % NSLOT
            for n in range(NF):
                pltpu.make_async_copy(
                    w.at[e, pl.ds(k * KC, KC), pl.ds(n * KC, KC)],
                    ring.at[slot, pl.ds(n * KC, KC)], ring_sem.at[slot]).start()

    def start_p2(p):
        c = p // (NE // 2)
        j = p % (NE // 2)
        for m in range(2):
            slot = (2 * (P1 + p) + m) % NSLOT
            pltpu.make_async_copy(
                wd_hbm.at[2 * j + m, :, pl.ds(pl.multiple_of(c * KC, KC), KC)], ring.at[slot], ring_sem.at[slot]).start()

    def wait_slot(slot):
        pltpu.make_async_copy(wd_hbm.at[0, :, pl.ds(0, KC)], ring.at[slot], ring_sem.at[slot]).wait()

    for s in range(AHEAD):
        start_p1(s)

    barrier = pltpu.get_barrier_semaphore()
    for d in (sibling, partner, diag):
        pl.semaphore_signal(barrier, inc=1, device_id={"ep": d}, device_id_type=pl.DeviceIdType.MESH)

    for d in range(4):
        h_all[:, d * PAD + TOK:(d + 1) * PAD, :] = jnp.zeros((NK, PAD - TOK, KC), bf16)

    for c in ins:
        c.wait()
    my_rows = pl.ds(pl.multiple_of(me * PAD, PAD), TOK)
    ssq = jnp.zeros((TOK, 1), f32)
    for k in range(NK):
        xc = xv[:, k * KC:(k + 1) * KC].astype(f32)
        ssq = ssq + jnp.sum(xc * xc, axis=1, keepdims=True)
    inv = lax.rsqrt(ssq * (1.0 / (NK * KC)) + EPS)
    for k in range(NK):
        xc = xv[:, k * KC:(k + 1) * KC].astype(f32)
        h_all[k, my_rows, :] = (xc * inv * gv[:, k * KC:(k + 1) * KC].astype(f32)).astype(bf16)

    pl.semaphore_wait(barrier, 3)

    def h_copy(k, owner, target, ss, rs):
        rows = pl.ds(pl.multiple_of(owner * PAD, PAD), TOK)
        return pltpu.make_async_remote_copy(
            src_ref=h_all.at[k, rows], dst_ref=h_all.at[k, rows], send_sem=h_send.at[k, ss], recv_sem=h_recv.at[k, rs],
            device_id={"ep": target}, device_id_type=pl.DeviceIdType.MESH)

    for k in range(NK):
        h_copy(k, me, partner, 1, 1).start()
        h_copy(k, me, sibling, 0, 0).start()

    logits = jnp.zeros((64, TOK), f32)
    for k in range(NK):
        logits = logits + lax.dot_general(
            wrv[:, k * KC:(k + 1) * KC], h_all[k, my_rows, :], (((1,), (1,)), ((), ())), preferred_element_type=f32)
    e_iota = lax.broadcasted_iota(i32, (64, TOK), 0)
    hit = jnp.zeros((64, TOK), f32)
    for j in range(6):
        hit = hit + jnp.where(idv[j:j + 1, :] == e_iota, 1.0, 0.0)
    ex = jnp.exp(logits - jnp.max(logits, axis=0, keepdims=True))
    prob = ex / jnp.sum(ex, axis=0, keepdims=True)
    picked = prob * hit
    gates = picked / jnp.sum(picked, axis=0, keepdims=True)
    upper = (lax.broadcasted_iota(i32, (TOK, TOK), 0) < lax.broadcasted_iota(i32, (TOK, TOK), 1)).astype(f32).astype(bf16)
    before = jnp.dot(hit.astype(bf16), upper, preferred_element_type=f32)
    pos = jnp.where(hit > 0.5, before + (core * CAP).astype(f32), -1.0)
    for d in range(4):
        info_own[d, 0] = jnp.full((NE, PAD), -1.0, f32)
        info_own[d, 1] = jnp.zeros((NE, PAD), f32)
        info_own[d, 0, :, 0:TOK] = pos[d * NE:(d + 1) * NE]
        info_own[d, 1, :, 0:TOK] = gates[d * NE:(d + 1) * NE]

    def i_copy(idx, target):
        return pltpu.make_async_remote_copy(
            src_ref=info_own.at[target], dst_ref=info_all.at[me], send_sem=i_send.at[idx], recv_sem=i_recv.at[idx],
            device_id={"ep": target}, device_id_type=pl.DeviceIdType.MESH)

    peers = (sibling, partner, diag)
    for idx, d in enumerate(peers):
        i_copy(idx, d).start()
    info_all[me] = info_own[me]
    for idx, d in enumerate(peers):
        i_copy(idx, d).wait_recv()

    r_iota = lax.broadcasted_iota(i32, (CROW, 2 * PAD), 0).astype(f32)
    for ch in range(2):
        prow = jnp.concatenate([info_all[2 * ch, 0], info_all[2 * ch + 1, 0]], axis=1)
        for q in range(NE // 2):
            pair = [jnp.where(r_iota == prow[2 * q + i:2 * q + i + 1, :], 1.0, 0.0) for i in range(2)]
            gat[ch, q * EROW:(q + 1) * EROW, :] = jnp.concatenate(pair, axis=0).astype(bf16)

    acc[...] = jnp.zeros_like(acc)

    def build_combine():
        lane = lax.broadcasted_iota(i32, (NE, SLOTS), 1)
        expand = (lane // CROW == lax.broadcasted_iota(i32, (NE, SLOTS), 0)).astype(f32).astype(bf16)
        lane1 = lax.broadcasted_iota(i32, (TOK, SLOTS), 1)
        slot_r = (lane1 % CROW).astype(f32)
        for d in range(4):
            ptok = jnp.transpose(info_all[d, 0])[:TOK]
            wtok = jnp.transpose(info_all[d, 1])[:TOK]
            pexp = jnp.dot(ptok.astype(bf16), expand, preferred_element_type=f32)
            sel = pexp == slot_r
            rows = slice((d % 2) * TOK, (d % 2 + 1) * TOK)
            rest = wtok
            for i in range(3):
                part = rest.astype(bf16)
                rest = rest - part.astype(f32)
                wexp = jnp.dot(part, expand, preferred_element_type=f32)
                cmb[i, d // 2, rows, :] = jnp.where(sel, wexp, 0.0).astype(bf16)

    def k_body(gk, _):
        g = gk // NK
        k = gk % NK

        @pl.when(g == 0)
        def _():
            h_copy(k, partner, sibling, 1, 1).wait_recv()
            h_copy(k, partner, sibling, 2, 2).start()
            h_copy(k, sibling, sibling, 0, 0).wait_recv()
            h_copy(k, diag, sibling, 2, 2).wait_recv()

        outs = [jnp.dot(gat[ch, pl.ds(pl.multiple_of(g * (GE * CROW), GE * CROW), GE * CROW), :],
                        h_all[k, ch * 2 * PAD:(ch + 1) * 2 * PAD, :], preferred_element_type=f32) for ch in range(2)]
        for e in range(GE):
            xg[e] = jnp.concatenate([o[e * CROW:(e + 1) * CROW] for o in outs], axis=0).astype(bf16)

        def e_body(e, _):
            s = gk * GE + e
            xe = xg[e]
            for m in range(2):
                slot = (2 * s + m) % NSLOT
                wait_slot(slot)
                for n in range(NF):
                    rows = pl.ds(pl.multiple_of(((e * 2 + m) * NF + n) * EROW, EROW), EROW)
                    acc[rows, :] = acc[rows, :] + jnp.dot(
                        xe, ring[slot, n * KC:(n + 1) * KC, :], preferred_element_type=f32)

            @pl.when(s + AHEAD < P1)
            def _():
                start_p1(s + AHEAD)

            @pl.when(s + AHEAD >= P1)
            def _():
                start_p2(s + AHEAD - P1)
            return 0

        lax.fori_loop(0, GE, e_body, 0)

        @pl.when(k == NK - 1)
        def _():
            def s_body(e, _):
                for n in range(NF):
                    rg = pl.ds(pl.multiple_of(((e * 2) * NF + n) * EROW, EROW), EROW)
                    ru = pl.ds(pl.multiple_of(((e * 2 + 1) * NF + n) * EROW, EROW), EROW)
                    a = jax.nn.silu(acc[rg, :]) * acc[ru, :]
                    act[g * GE + e, :, n * KC:(n + 1) * KC] = a.astype(bf16)
                    acc[rg, :] = jnp.zeros((EROW, KC), f32)
                    acc[ru, :] = jnp.zeros((EROW, KC), f32)
                return 0
            lax.fori_loop(0, GE, s_body, 0)

        @pl.when(gk == 2 * NK)
        def _():
            build_combine()
        return 0

    lax.fori_loop(0, (NE // GE) * NK, k_body, 0)

    def part_rows(slot, mine_chip, which):
        return pl.ds(pl.multiple_of(((slot * 2 + mine_chip) * 2 + which) * TOK, TOK), TOK)

    def s_copy(c, i):
        return pltpu.make_async_remote_copy(
            src_ref=acc.at[part_rows(c % 2, i, 1 - core)], dst_ref=sib.at[c, i],
            send_sem=s_send.at[c, i], recv_sem=s_recv.at[c, i],
            device_id={"ep": sibling}, device_id_type=pl.DeviceIdType.MESH)

    def r_copy(c):
        return pltpu.make_async_remote_copy(
            src_ref=sib.at[c, 0], dst_ref=rem.at[c], send_sem=r_send.at[c], recv_sem=r_recv.at[c],
            device_id={"ep": partner}, device_id_type=pl.DeviceIdType.MESH)

    def relay(c):
        s_copy(c, 0).wait_recv()
        sib[c, 0] = sib[c, 0] + acc[part_rows(c % 2, 0, core), :]
        r_copy(c).start()
        s_copy(c, 1).wait_recv()
        sib[c, 1] = sib[c, 1] + acc[part_rows(c % 2, 1, core), :]

    def combine(c):
        @pl.when(c >= 2)
        def _():
            s_copy(c - 2, 0).wait_send()
            s_copy(c - 2, 1).wait_send()
        for i in range(2):
            ch = (1 - chip) if i == 0 else chip
            tot = jnp.zeros((2 * TOK, KC), f32)
            for q in range(3):
                tot = tot + jnp.dot(cmb[q, ch], yb[ch], preferred_element_type=f32)
            acc[pl.ds(pl.multiple_of(((c % 2) * 2 + i) * 2 * TOK, 2 * TOK), 2 * TOK), :] = tot
            s_copy(c, i).start()

    def d_body(p, _):
        c = p // (NE // 2)
        j = p % (NE // 2)
        ys = []
        for m in range(2):
            slot = (2 * (P1 + p) + m) % NSLOT
            wait_slot(slot)
            ys.append(jnp.dot(act[2 * j + m], ring[slot], preferred_element_type=f32))
        for ch in range(2):
            yb[ch, pl.ds(pl.multiple_of(j * EROW, EROW), EROW), :] = jnp.concatenate(
                [y[ch * CROW:(ch + 1) * CROW] for y in ys], axis=0).astype(bf16)

        @pl.when(p + AHEAD < P2)
        def _():
            start_p2(p + AHEAD)

        @pl.when((j == 1) & (c > 0))
        def _():
            relay(c - 1)

        @pl.when(j == NE // 2 - 1)
        def _():
            combine(c)
        return 0

    lax.fori_loop(0, P2, d_body, 0)
    relay(NK - 1)

    for c in range(NK):
        r_copy(c).wait_recv()
        cols = slice(c * KC, (c + 1) * KC)
        out_ref[:, cols] = (xv[:, cols].astype(f32) + (sib[c, 1] + rem[c])).astype(bf16)

    for k in range(NK):
        h_copy(k, me, sibling, 0, 0).wait_send()
        h_copy(k, me, partner, 1, 1).wait_send()
        h_copy(k, partner, sibling, 2, 2).wait_send()
    for idx, d in enumerate(peers):
        i_copy(idx, d).wait_send()
    for c in range(NK):
        r_copy(c).wait_send()
    for c in range(NK - 2, NK):
        for i in range(2):
            s_copy(c, i).wait_send()


def solution(mesh):
    def local_block(x_in, norm_gain, w_router, expert_ids, w_gate, w_up, w_down):
        tokens, hidden = x_in.shape
        dma = pltpu.SemaphoreType.DMA
        return pl.pallas_call(
            kernel,
            out_shape=jax.ShapeDtypeStruct((tokens, hidden), bf16),
            in_specs=[pl.BlockSpec(memory_space=pl.ANY)] * 7,
            out_specs=pl.BlockSpec(memory_space=pltpu.VMEM),
            scratch_shapes=[
                pltpu.VMEM((TOK, NK * KC), bf16),
                pltpu.VMEM((1, NK * KC), bf16),
                pltpu.VMEM((64, NK * KC), bf16),
                pltpu.VMEM((6, TOK), i32),
                pltpu.VMEM((NK, 4 * PAD, KC), bf16),
                pltpu.VMEM((4, 2, NE, PAD), f32),
                pltpu.VMEM((4, 2, NE, PAD), f32),
                pltpu.VMEM((2, SLOTS, 2 * PAD), bf16),
                pltpu.VMEM((3, 2, 2 * TOK, SLOTS), bf16),
                pltpu.VMEM((GE * 2 * NF * EROW, KC), f32),
                pltpu.VMEM((NE, EROW, FF), bf16),
                pltpu.VMEM((NSLOT, FF, KC), bf16),
                pltpu.VMEM((GE, EROW, KC), bf16),
                pltpu.VMEM((2, SLOTS, KC), bf16),
                pltpu.VMEM((NK, 2, TOK, KC), f32),
                pltpu.VMEM((NK, TOK, KC), f32),
                dma((4,)), dma((NSLOT,)),
                dma((NK, 3)), dma((NK, 3)),
                dma((3,)), dma((3,)),
                dma((NK, 2)), dma((NK, 2)),
                dma((NK,)), dma((NK,)),
            ],
            compiler_params=pltpu.CompilerParams(
                collective_id=0, has_side_effects=True, vmem_limit_bytes=67_043_328),
            name="moe_step",
        )(x_in, norm_gain.reshape(1, hidden), w_router.T, expert_ids.T, w_gate, w_up, w_down)

    tok_spec = P(("dp", "ep"), None)
    expert_spec = P("ep", None, None)
    return jax.shard_map(local_block, mesh=mesh, in_specs=(tok_spec, P(None), P(None, None), tok_spec, expert_spec, expert_spec, expert_spec), out_specs=tok_spec, check_vma=False)
```

```python
import functools

import jax
import jax.numpy as jnp
from jax import lax
from jax.experimental import pallas as pl
from jax.experimental.pallas import tpu as pltpu
from jax.sharding import PartitionSpec as P

EPS = 1e-6
TOK = 192
PAD = 256
CAP = 36
EROW = 4 * CAP
NE = 16
GE = 4
KC = 512
NK = 5
FF = 1536
NF = 3
NSLOT = 16
AHEAD = NSLOT // 2
P1 = NE * NK
P2 = NK * NE // 2
PROW = 2 * CAP
DSLOT = NE // 2 * PROW
MISS = -100.0
f32, bf16, i32 = jnp.float32, jnp.bfloat16, jnp.int32


def kernel(x_hbm, gain_hbm, wr_hbm, ids_hbm, wg_hbm, wu_hbm, wd_hbm, out_ref,
           xv, gv, wrv, idv, h_all, pos_own, gate_own, pos_all, gate_all, gat, cmb, acc, act, ring, xg, yb, sib, rem,
           in_sem, ring_sem, h_send, h_recv, p_send, p_recv, g_send, g_recv, s_send, s_recv, r_send, r_recv):
    me = lax.axis_index("ep")
    chip = me // 2
    core = me % 2
    sibling = chip * 2 + (1 - core)
    partner = (1 - chip) * 2 + core
    diag = (1 - chip) * 2 + (1 - core)
    peers = (partner, diag, sibling)

    ins = [pltpu.make_async_copy(s, d, in_sem.at[i]) for i, (s, d) in enumerate(
        ((ids_hbm, idv), (x_hbm, xv), (gain_hbm, gv), (wr_hbm, wrv)))]
    for c in ins:
        c.start()

    def start_p1(s):
        g = s // (NK * GE)
        k = (s % (NK * GE)) // GE
        e = g * GE + s % GE
        for m, w in enumerate((wg_hbm, wu_hbm)):
            slot = (2 * s + m) % NSLOT
            for n in range(NF):
                pltpu.make_async_copy(
                    w.at[e, pl.ds(k * KC, KC), pl.ds(n * KC, KC)],
                    ring.at[slot, pl.ds(n * KC, KC)], ring_sem.at[slot]).start()

    def start_p2(p):
        c = p // (NE // 2)
        j = p % (NE // 2)
        for m in range(2):
            slot = (2 * (P1 + p) + m) % NSLOT
            pltpu.make_async_copy(
                wd_hbm.at[2 * j + m, :, pl.ds(pl.multiple_of(c * KC, KC), KC)], ring.at[slot], ring_sem.at[slot]).start()

    def wait_slot(slot):
        pltpu.make_async_copy(wd_hbm.at[0, :, pl.ds(0, KC)], ring.at[slot], ring_sem.at[slot]).wait()

    barrier = pltpu.get_barrier_semaphore()
    for d in peers:
        pl.semaphore_signal(barrier, inc=1, device_id={"ep": d}, device_id_type=pl.DeviceIdType.MESH)

    for d in range(4):
        h_all[:, d * PAD + TOK:(d + 1) * PAD, :] = jnp.zeros((NK, PAD - TOK, KC), bf16)
    for d in range(4):
        pos_own[d] = jnp.full((NE, PAD), MISS, f32)
        gate_own[d] = jnp.zeros((NE, PAD), f32)

    ins[0].wait()
    e_iota = lax.broadcasted_iota(i32, (64, TOK), 0)
    hit = jnp.zeros((64, TOK), f32)
    for j in range(6):
        hit = hit + jnp.where(idv[j:j + 1, :] == e_iota, 1.0, 0.0)
    upper = (lax.broadcasted_iota(i32, (TOK, TOK), 0) < lax.broadcasted_iota(i32, (TOK, TOK), 1)).astype(f32).astype(bf16)
    before = jnp.dot(hit.astype(bf16), upper, preferred_element_type=f32)
    pos = jnp.where(hit > 0.5, before, MISS)
    for d in range(4):
        pos_own[d, :, 0:TOK] = pos[d * NE:(d + 1) * NE]

    for c in ins[1:]:
        c.wait()
    for s in range(AHEAD):
        start_p1(s)
    my_rows = pl.ds(pl.multiple_of(me * PAD, PAD), TOK)
    ssq = jnp.zeros((TOK, 1), f32)
    for k in range(NK):
        xc = xv[:, k * KC:(k + 1) * KC].astype(f32)
        ssq = ssq + jnp.sum(xc * xc, axis=1, keepdims=True)
    inv = lax.rsqrt(ssq * (1.0 / (NK * KC)) + EPS)
    for k in range(NK):
        xc = xv[:, k * KC:(k + 1) * KC].astype(f32)
        h_all[k, my_rows, :] = (xc * inv * gv[:, k * KC:(k + 1) * KC].astype(f32)).astype(bf16)

    pl.semaphore_wait(barrier, 3)

    def small_copy(own, everyone, ss, rs, idx, target):
        return pltpu.make_async_remote_copy(
            src_ref=own.at[target], dst_ref=everyone.at[me], send_sem=ss.at[idx], recv_sem=rs.at[idx],
            device_id={"ep": target}, device_id_type=pl.DeviceIdType.MESH)

    def pos_copy(idx):
        return small_copy(pos_own, pos_all, p_send, p_recv, idx, peers[idx])

    def gate_copy(idx):
        return small_copy(gate_own, gate_all, g_send, g_recv, idx, peers[idx])

    def h_copy(k, owner, target, ss):
        rows = pl.ds(pl.multiple_of(owner * PAD, PAD), TOK)
        return pltpu.make_async_remote_copy(
            src_ref=h_all.at[k, rows], dst_ref=h_all.at[k, rows], send_sem=h_send.at[k, ss], recv_sem=h_recv.at[k, ss],
            device_id={"ep": target}, device_id_type=pl.DeviceIdType.MESH)

    def own_to_sibling(k):
        return h_copy(k, me, sibling, 0)

    def own_to_partner(k):
        return h_copy(k, me, partner, 1)

    def hand_on(k):
        return h_copy(k, partner, sibling, 2)

    for idx in range(3):
        pos_copy(idx).start()
    for k in range(NK):
        own_to_partner(k).start()
        own_to_sibling(k).start()

    logits = jnp.zeros((64, TOK), f32)
    for k in range(NK):
        logits = logits + lax.dot_general(
            wrv[:, k * KC:(k + 1) * KC], h_all[k, my_rows, :], (((1,), (1,)), ((), ())), preferred_element_type=f32)
    ex = jnp.exp(logits - jnp.max(logits, axis=0, keepdims=True))
    prob = ex / jnp.sum(ex, axis=0, keepdims=True)
    picked = prob * hit
    gates = picked / jnp.sum(picked, axis=0, keepdims=True)
    for d in range(4):
        gate_own[d, :, 0:TOK] = gates[d * NE:(d + 1) * NE]
    for idx in range(3):
        gate_copy(idx).start()
    pos_all[me] = pos_own[me]
    gate_all[me] = gate_own[me]
    acc[...] = jnp.zeros_like(acc)

    for idx in range(3):
        pos_copy(idx).wait_recv()

    ri = lax.broadcasted_iota(i32, (PROW, PAD), 0)
    r_iota = ri.astype(f32)
    low = ri < CAP
    for d in range(4):
        for q in range(NE // 4):
            two = []
            for jj in range(2):
                e0 = 4 * q + 2 * jj
                ea, eb = e0 + d % 2, e0 + 1 - d % 2
                want = jnp.where(low, pos_all[d, ea:ea + 1, :], pos_all[d, eb:eb + 1, :] + CAP)
                two.append(jnp.where(r_iota == want, 1.0, 0.0))
            gat[d, q * EROW:(q + 1) * EROW, :] = jnp.concatenate(two, axis=0).astype(bf16)

    own_to_partner(0).wait_recv()
    hand_on(0).start()

    def build_combine():
        for idx in range(3):
            gate_copy(idx).wait_recv()
        le = lax.broadcasted_iota(i32, (NE, DSLOT), 1)
        ee = lax.broadcasted_iota(i32, (NE, DSLOT), 0)
        lane = lax.broadcasted_iota(i32, (TOK, DSLOT), 1) % PROW
        slot_r = jnp.where(lane < CAP, lane, lane - CAP).astype(f32)
        for d in range(4):
            swap = jnp.where(le % PROW < CAP, d % 2, 1 - d % 2)
            expand = (le // PROW * 2 + swap == ee).astype(f32).astype(bf16)
            ptok = jnp.transpose(pos_all[d])[:TOK]
            wtok = jnp.transpose(gate_all[d])[:TOK]
            pexp = jnp.dot(ptok.astype(bf16), expand, preferred_element_type=f32)
            sel = pexp == slot_r
            rest = wtok
            for i in range(3):
                part = rest.astype(bf16)
                rest = rest - part.astype(f32)
                wexp = jnp.dot(part, expand, preferred_element_type=f32)
                cmb[d, i] = jnp.where(sel, wexp, 0.0).astype(bf16)

    half = lax.broadcasted_iota(i32, (PROW, KC), 0) < CAP

    def k_body(gk, _):
        g = gk // NK
        k = gk % NK

        @pl.when(g == 0)
        def _():
            own_to_sibling(k).wait_recv()
            hand_on(k).wait_recv()

        outs = [jnp.dot(gat[d, pl.ds(pl.multiple_of(g * EROW, EROW), EROW), :],
                        h_all[k, d * PAD:(d + 1) * PAD, :], preferred_element_type=f32) for d in range(4)]
        for jj in range(2):
            o = [v[jj * PROW:(jj + 1) * PROW] for v in outs]
            xg[2 * jj] = jnp.concatenate(
                [jnp.where(half, o[0], o[1]), jnp.where(half, o[2], o[3])], axis=0).astype(bf16)
            xg[2 * jj + 1] = jnp.concatenate(
                [jnp.where(half, o[1], o[0]), jnp.where(half, o[3], o[2])], axis=0).astype(bf16)

        for jj in range(GE // 2):
            s0 = gk * GE + 2 * jj
            for i in range(4):
                wait_slot((2 * s0 + i) % NSLOT)
            for i in range(2):
                e = 2 * jj + i
                for m in range(2):
                    slot = (2 * s0 + 2 * i + m) % NSLOT
                    for n in range(NF):
                        r = ((e * 2 + m) * NF + n) * EROW
                        acc[r:r + EROW, :] = acc[r:r + EROW, :] + jnp.dot(
                            xg[e], ring[slot, n * KC:(n + 1) * KC, :], preferred_element_type=f32)

            for i in range(2):
                s = s0 + i

                @pl.when(s + AHEAD < P1)
                def _():
                    start_p1(s + AHEAD)

                @pl.when(s + AHEAD >= P1)
                def _():
                    start_p2(s + AHEAD - P1)

            if jj == 0:
                @pl.when(gk < NK - 1)
                def _():
                    own_to_partner(k + 1).wait_recv()
                    hand_on(k + 1).start()

        @pl.when(k == NK - 1)
        def _():
            def s_body(e, _):
                for n in range(NF):
                    rg = pl.ds(pl.multiple_of(((e * 2) * NF + n) * EROW, EROW), EROW)
                    ru = pl.ds(pl.multiple_of(((e * 2 + 1) * NF + n) * EROW, EROW), EROW)
                    a = jax.nn.silu(acc[rg, :]) * acc[ru, :]
                    act[g * GE + e, :, n * KC:(n + 1) * KC] = a.astype(bf16)
                    acc[rg, :] = jnp.zeros((EROW, KC), f32)
                    acc[ru, :] = jnp.zeros((EROW, KC), f32)
                return 0
            lax.fori_loop(0, GE, s_body, 0)

        @pl.when(gk == 2 * NK)
        def _():
            build_combine()
        return 0

    lax.fori_loop(0, (NE // GE) * NK, k_body, 0)

    def part_rows(slot, where, which):
        return pl.ds(pl.multiple_of(((slot * 2 + where) * 2 + which) * TOK, TOK), TOK)

    def s_copy(c, i):
        return pltpu.make_async_remote_copy(
            src_ref=acc.at[part_rows(c % 2, i, 1 - core)], dst_ref=sib.at[c, i],
            send_sem=s_send.at[c, i], recv_sem=s_recv.at[c, i],
            device_id={"ep": sibling}, device_id_type=pl.DeviceIdType.MESH)

    def r_copy(c):
        return pltpu.make_async_remote_copy(
            src_ref=sib.at[c, 0], dst_ref=rem.at[c], send_sem=r_send.at[c], recv_sem=r_recv.at[c],
            device_id={"ep": partner}, device_id_type=pl.DeviceIdType.MESH)

    def relay(c):
        s_copy(c, 0).wait_recv()
        sib[c, 0] = sib[c, 0] + acc[part_rows(c % 2, 0, core), :]
        r_copy(c).start()
        s_copy(c, 1).wait_recv()
        sib[c, 1] = sib[c, 1] + acc[part_rows(c % 2, 1, core), :]

    def combine(c):
        @pl.when(c >= 2)
        def _():
            s_copy(c - 2, 0).wait_send()
            s_copy(c - 2, 1).wait_send()
        for i in range(2):
            ch = (1 - chip) if i == 0 else chip
            for w in range(2):
                d = ch * 2 + w
                tot = jnp.dot(cmb[d, 0], yb[d], preferred_element_type=f32)
                for q in range(1, 3):
                    tot = tot + jnp.dot(cmb[d, q], yb[d], preferred_element_type=f32)
                acc[part_rows(c % 2, i, w), :] = tot
            s_copy(c, i).start()

    def d_body(t, _):
        c = t // (NE // 4)
        q = t % (NE // 4)
        ys = []
        for i in range(4):
            wait_slot((2 * P1 + 4 * t + i) % NSLOT)
        for i in range(4):
            ys.append(jnp.dot(act[4 * q + i], ring[(2 * P1 + 4 * t + i) % NSLOT], preferred_element_type=f32))
        for ch in range(2):
            r0, r1 = ch * PROW, (ch + 1) * PROW
            for w in range(2):
                rows = [jnp.where(half, ys[2 * jj + w][r0:r1], ys[2 * jj + 1 - w][r0:r1]) for jj in range(2)]
                yb[2 * ch + w, pl.ds(pl.multiple_of(q * EROW, EROW), EROW), :] = jnp.concatenate(
                    rows, axis=0).astype(bf16)

        for i in range(2):
            p = 2 * t + i

            @pl.when(p + AHEAD < P2)
            def _():
                start_p2(p + AHEAD)

        @pl.when((q == 0) & (c > 0))
        def _():
            relay(c - 1)

        @pl.when(q == NE // 4 - 1)
        def _():
            combine(c)
        return 0

    lax.fori_loop(0, P2 // 2, d_body, 0)
    relay(NK - 1)

    for c in range(NK):
        r_copy(c).wait_recv()
        cols = slice(c * KC, (c + 1) * KC)
        out_ref[:, cols] = (xv[:, cols].astype(f32) + (sib[c, 1] + rem[c])).astype(bf16)

    for k in range(NK):
        own_to_sibling(k).wait_send()
        own_to_partner(k).wait_send()
        hand_on(k).wait_send()
    for idx in range(3):
        pos_copy(idx).wait_send()
        gate_copy(idx).wait_send()
    for c in range(NK):
        r_copy(c).wait_send()
    for c in range(NK - 2, NK):
        for i in range(2):
            s_copy(c, i).wait_send()


def solution(mesh):
    def local_block(x_in, norm_gain, w_router, expert_ids, w_gate, w_up, w_down):
        tokens, hidden = x_in.shape
        dma = pltpu.SemaphoreType.DMA
        return pl.pallas_call(
            kernel,
            out_shape=jax.ShapeDtypeStruct((tokens, hidden), bf16),
            in_specs=[pl.BlockSpec(memory_space=pl.ANY)] * 7,
            out_specs=pl.BlockSpec(memory_space=pltpu.VMEM),
            scratch_shapes=[
                pltpu.VMEM((TOK, NK * KC), bf16),
                pltpu.VMEM((1, NK * KC), bf16),
                pltpu.VMEM((64, NK * KC), bf16),
                pltpu.VMEM((6, TOK), i32),
                pltpu.VMEM((NK, 4 * PAD, KC), bf16),
                pltpu.VMEM((4, NE, PAD), f32),
                pltpu.VMEM((4, NE, PAD), f32),
                pltpu.VMEM((4, NE, PAD), f32),
                pltpu.VMEM((4, NE, PAD), f32),
                pltpu.VMEM((4, DSLOT, PAD), bf16),
                pltpu.VMEM((4, 3, TOK, DSLOT), bf16),
                pltpu.VMEM((GE * 2 * NF * EROW, KC), f32),
                pltpu.VMEM((NE, EROW, FF), bf16),
                pltpu.VMEM((NSLOT, FF, KC), bf16),
                pltpu.VMEM((GE, EROW, KC), bf16),
                pltpu.VMEM((4, DSLOT, KC), bf16),
                pltpu.VMEM((NK, 2, TOK, KC), f32),
                pltpu.VMEM((NK, TOK, KC), f32),
                dma((4,)), dma((NSLOT,)),
                dma((NK, 3)), dma((NK, 3)),
                dma((3,)), dma((3,)),
                dma((3,)), dma((3,)),
                dma((NK, 2)), dma((NK, 2)),
                dma((NK,)), dma((NK,)),
            ],
            compiler_params=pltpu.CompilerParams(
                collective_id=0, has_side_effects=True, vmem_limit_bytes=67_043_328),
            name="moe_step",
        )(x_in, norm_gain.reshape(1, hidden), w_router.T, expert_ids.T, w_gate, w_up, w_down)

    tok_spec = P(("dp", "ep"), None)
    expert_spec = P("ep", None, None)
    return jax.shard_map(local_block, mesh=mesh, in_specs=(tok_spec, P(None), P(None, None), tok_spec, expert_spec, expert_spec, expert_spec), out_specs=tok_spec, check_vma=False)
```

```python
import jax
import jax.numpy as jnp
from jax import lax
from jax.experimental import pallas as pl
from jax.experimental.pallas import tpu as pltpu
from jax.sharding import PartitionSpec as P

EPS = 1e-6
TOK = 192
PAD = 256
CAP = 36
PROW = 2 * CAP
GROW = 80
EROW = 4 * CAP
NE = 16
DSLOT = NE // 2 * PROW
MISS = -100.0
KC = 512
NK = 5
FF = 1536
NF = 3
NSLOT = 16
AHEAD = NSLOT // 2
GROUPS = ((0, 4, 0, 4, 0), (20, 3, 4, 2, 2), (35, 3, 6, 2, 3), (50, 4, 8, 4, 4))
P1 = 70
CHUNKS = ((0, 256), (256, 256), (512, 512), (1024, 512), (1536, 512), (2048, 512))
NC = len(CHUNKS)
f32, bf16, i32 = jnp.float32, jnp.bfloat16, jnp.int32
MESH = pl.DeviceIdType.MESH


def kernel(x_hbm, gain_hbm, wr_hbm, ids_hbm, wg_hbm, wu_hbm, wd_hbm, out_hbm,
           xv, gv, wrv, idv, h_all, pos_own, gate_own, pos_all, gate_all, gat, cmb, acc, act, ring, xg, xs, xp, sa,
           yb, sib, rem,
           in_sem, out_sem, ring_sem, h_send, h_recv, p_send, p_recv, g_send, g_recv, x_send, x_recv, a_send, a_recv,
           s_send, s_recv, r_send, r_recv):
    me = lax.axis_index("ep")
    dp = lax.axis_index("dp")
    chip = me // 2
    core = me % 2
    sibling = chip * 2 + (1 - core)
    partner = (1 - chip) * 2 + core
    diag = (1 - chip) * 2 + (1 - core)
    peers = (partner, diag, sibling)
    twin = {"dp": 1 - dp, "ep": me}

    ins = [pltpu.make_async_copy(s, d, in_sem.at[i]) for i, (s, d) in enumerate(
        ((ids_hbm, idv), (x_hbm, xv), (gain_hbm, gv), (wr_hbm, wrv)))]
    for c in ins:
        c.start()

    def slot_of(s, i):
        return (2 * s + i) % NSLOT

    def fill_up(g, s):
        base, per, common, n_common, _ = GROUPS[g]
        t = s - base
        k, i = t // per, t % per
        e = common + i
        if n_common == 2:
            e = e + (i // 2) * (12 + g - 1 + 2 * dp - common - 2)
        for m, w in enumerate((wg_hbm, wu_hbm)):
            for n in range(NF):
                pltpu.make_async_copy(
                    w.at[e, pl.ds(k * KC, KC), pl.ds(n * KC, KC)],
                    ring.at[slot_of(s, m), pl.ds(n * KC, KC)], ring_sem.at[slot_of(s, m)]).start()

    def fill_down(c, s):
        col, width = CHUNKS[c]
        j = s - P1 - c * (NE // 2)
        for m in range(2):
            slot = slot_of(s, m)
            pltpu.make_async_copy(
                wd_hbm.at[2 * j + m, :, pl.ds(col, width)], ring.at[slot, :, pl.ds(0, width)], ring_sem.at[slot]).start()

    spans = [(GROUPS[g][0], GROUPS[g][0] + NK * GROUPS[g][1], lambda s, g=g: fill_up(g, s)) for g in range(4)]
    spans += [(P1 + c * (NE // 2), P1 + (c + 1) * (NE // 2), lambda s, c=c: fill_down(c, s)) for c in range(NC)]

    def fill(s, low, high):
        todo = [v for v in spans if v[0] <= high and low < v[1]]
        for a, b, fn in todo:
            if a <= low and high < b:
                fn(s)
            else:
                pl.when((s >= a) & (s < b))(lambda fn=fn: fn(s))

    def wait_up(slot):
        pltpu.make_async_copy(wd_hbm.at[0, :, pl.ds(0, KC)], ring.at[slot], ring_sem.at[slot]).wait()

    barrier = pltpu.get_barrier_semaphore()
    for d in peers:
        pl.semaphore_signal(barrier, inc=1, device_id={"ep": d}, device_id_type=MESH)
    pl.semaphore_signal(barrier, inc=1, device_id=twin, device_id_type=MESH)

    for d in range(4):
        h_all[:, d * PAD + TOK:(d + 1) * PAD, :] = jnp.zeros((NK, PAD - TOK, KC), bf16)
    for d in range(4):
        pos_own[d] = jnp.full((NE, PAD), MISS, f32)
        gate_own[d] = jnp.zeros((NE, PAD), f32)

    ins[0].wait()
    e_iota = lax.broadcasted_iota(i32, (64, TOK), 0)
    hit = jnp.zeros((64, TOK), f32)
    for j in range(6):
        hit = hit + jnp.where(idv[j:j + 1, :] == e_iota, 1.0, 0.0)
    upper = (lax.broadcasted_iota(i32, (TOK, TOK), 0) < lax.broadcasted_iota(i32, (TOK, TOK), 1)).astype(f32).astype(bf16)
    before = jnp.dot(hit.astype(bf16), upper, preferred_element_type=f32)
    pos = jnp.where(hit > 0.5, before, MISS)
    for d in range(4):
        pos_own[d, :, 0:TOK] = pos[d * NE:(d + 1) * NE]

    for c in ins[1:]:
        c.wait()
    for s in range(AHEAD):
        fill(s, s, s)
    my_rows = pl.ds(pl.multiple_of(me * PAD, PAD), TOK)
    ssq = jnp.zeros((TOK, 1), f32)
    for k in range(NK):
        xc = xv[:, k * KC:(k + 1) * KC].astype(f32)
        ssq = ssq + jnp.sum(xc * xc, axis=1, keepdims=True)
    inv = lax.rsqrt(ssq * (1.0 / (NK * KC)) + EPS)
    for k in range(NK):
        xc = xv[:, k * KC:(k + 1) * KC].astype(f32)
        h_all[k, my_rows, :] = (xc * inv * gv[:, k * KC:(k + 1) * KC].astype(f32)).astype(bf16)

    pl.semaphore_wait(barrier, 4)

    def small_copy(own, everyone, ss, rs, idx):
        return pltpu.make_async_remote_copy(
            src_ref=own.at[peers[idx]], dst_ref=everyone.at[me], send_sem=ss.at[idx], recv_sem=rs.at[idx],
            device_id={"ep": peers[idx]}, device_id_type=MESH)

    def pos_copy(idx):
        return small_copy(pos_own, pos_all, p_send, p_recv, idx)

    def gate_copy(idx):
        return small_copy(gate_own, gate_all, g_send, g_recv, idx)

    def h_copy(k, owner, target, ss):
        rows = pl.ds(pl.multiple_of(owner * PAD, PAD), TOK)
        return pltpu.make_async_remote_copy(
            src_ref=h_all.at[k, rows], dst_ref=h_all.at[k, rows], send_sem=h_send.at[k, ss], recv_sem=h_recv.at[k, ss],
            device_id={"ep": target}, device_id_type=MESH)

    def own_to_sibling(k):
        return h_copy(k, me, sibling, 0)

    def own_to_partner(k):
        return h_copy(k, me, partner, 1)

    def hand_on(k):
        return h_copy(k, partner, sibling, 2)

    def x_copy(k, i):
        return pltpu.make_async_remote_copy(
            src_ref=xs.at[k, 1 - dp, i], dst_ref=xp.at[k, i], send_sem=x_send.at[k, i], recv_sem=x_recv.at[k, i],
            device_id=twin, device_id_type=MESH)

    def a_copy(i):
        return pltpu.make_async_remote_copy(
            src_ref=sa.at[i], dst_ref=act.at[12 + 2 * dp + i], send_sem=a_send.at[i], recv_sem=a_recv.at[i],
            device_id=twin, device_id_type=MESH)

    for idx in range(3):
        pos_copy(idx).start()
    for k in range(NK):
        own_to_partner(k).start()
        own_to_sibling(k).start()

    logits = jnp.zeros((64, TOK), f32)
    for k in range(NK):
        logits = logits + lax.dot_general(
            wrv[:, k * KC:(k + 1) * KC], h_all[k, my_rows, :], (((1,), (1,)), ((), ())), preferred_element_type=f32)
    ex = jnp.exp(logits - jnp.max(logits, axis=0, keepdims=True))
    prob = ex / jnp.sum(ex, axis=0, keepdims=True)
    picked = prob * hit
    gates = picked / jnp.sum(picked, axis=0, keepdims=True)
    for d in range(4):
        gate_own[d, :, 0:TOK] = gates[d * NE:(d + 1) * NE]
    for idx in range(3):
        gate_copy(idx).start()
    pos_all[me] = pos_own[me]
    gate_all[me] = gate_own[me]

    for idx in range(3):
        pos_copy(idx).wait_recv()

    ri = lax.broadcasted_iota(i32, (GROW, PAD), 0)
    r_iota = ri.astype(f32)
    low = ri < CAP
    for d in range(4):
        for j in range(NE // 2):
            ea, eb = 2 * j + d % 2, 2 * j + 1 - d % 2
            want = jnp.where(low, pos_all[d, ea:ea + 1, :], pos_all[d, eb:eb + 1, :] + CAP)
            gat[d, j] = jnp.where(r_iota == want, 1.0, 0.0).astype(bf16)

    own_to_partner(0).wait_recv()
    hand_on(0).start()

    def build_combine():
        for idx in range(3):
            gate_copy(idx).wait_recv()
        le = lax.broadcasted_iota(i32, (NE, DSLOT), 1)
        ee = lax.broadcasted_iota(i32, (NE, DSLOT), 0)
        lane = lax.broadcasted_iota(i32, (TOK, DSLOT), 1) % PROW
        slot_r = jnp.where(lane < CAP, lane, lane - CAP).astype(f32)
        for d in range(4):
            swap = jnp.where(le % PROW < CAP, d % 2, 1 - d % 2)
            expand = (le // PROW * 2 + swap == ee).astype(f32).astype(bf16)
            ptok = jnp.transpose(pos_all[d])[:TOK]
            wtok = jnp.transpose(gate_all[d])[:TOK]
            pexp = jnp.dot(ptok.astype(bf16), expand, preferred_element_type=f32)
            sel = pexp == slot_r
            rest = wtok
            for i in range(3):
                part = rest.astype(bf16)
                rest = rest - part.astype(f32)
                wexp = jnp.dot(part, expand, preferred_element_type=f32)
                cmb[d, i] = jnp.where(sel, wexp, 0.0).astype(bf16)

    half = lax.broadcasted_iota(i32, (PROW, KC), 0) < CAP

    def gather(k, pair, n_pair, store):
        outs = [jnp.dot(gat[d, pair:pair + n_pair].reshape(n_pair * GROW, PAD),
                        h_all[k, d * PAD:(d + 1) * PAD, :], preferred_element_type=f32) for d in range(4)]
        for jj in range(n_pair):
            o = [v[jj * GROW:jj * GROW + PROW] for v in outs]
            store(jj, 0, jnp.concatenate(
                [jnp.where(half, o[0], o[1]), jnp.where(half, o[2], o[3])], axis=0).astype(bf16))
            store(jj, 1, jnp.concatenate(
                [jnp.where(half, o[1], o[0]), jnp.where(half, o[3], o[2])], axis=0).astype(bf16))

    def k_step(g, k, mode):
        base, per, common, n_common, pair = GROUPS[g]
        static = isinstance(k, int)
        s0 = base + k * per
        lo, hi = (s0, s0) if static else (base + per, base + 3 * per)

        if g == 0:
            own_to_sibling(k).wait_recv()
            hand_on(k).wait_recv()
        if n_common == 2:
            x_copy(k, g - 1).wait_recv()
            if g == 1:
                x_copy(k, 1).start()

        def put(jj, i, v):
            xg[2 * jj + i] = v
        gather(k, pair, n_common // 2, put)
        if g == 0:
            def put_shared(jj, i, v):
                xs[k, jj, i] = v
            gather(k, 6, 2, put_shared)
        if g == 0:
            x_copy(k, 0).start()

        blocks = ((0, 1), (2, 3)) if g == 0 else (tuple(range(per)),)
        for b, block in enumerate(blocks):
            for i in block:
                for m in range(2):
                    wait_up(slot_of(s0 + i, m))
            for i in block:
                shared = i >= n_common
                lhs = jnp.concatenate([xs[k, dp, g - 1], xp[k, g - 1]], axis=0) if shared else xg[i]
                rows = 2 * EROW if shared else EROW
                for n in range(NF):
                    val = []
                    for m in range(2):
                        r = jnp.dot(lhs, ring[slot_of(s0 + i, m), n * KC:(n + 1) * KC, :], preferred_element_type=f32)
                        at = ((i if not shared else 2) * 6) * EROW + (m * NF + n) * rows
                        if mode == "first":
                            acc[at:at + rows, :] = r
                        elif mode == "middle":
                            acc[at:at + rows, :] = acc[at:at + rows, :] + r
                        else:
                            val.append(acc[at:at + rows, :] + r)
                    if mode == "last":
                        a = (jax.nn.silu(val[0]) * val[1]).astype(bf16)
                        cols = slice(n * KC, (n + 1) * KC)
                        if shared:
                            act[12 + 2 * dp + g - 1, :, cols] = a[:EROW]
                            sa[g - 1, :, cols] = a[EROW:]
                        else:
                            act[common + i, :, cols] = a
            for i in block:
                fill(s0 + i + AHEAD, lo + i + AHEAD, hi + i + AHEAD)
            if g == 0 and b == 0:
                if not static or k < NK - 1:
                    own_to_partner(k + 1).wait_recv()
                    hand_on(k + 1).start()
        if mode == "last" and n_common == 2:
            a_copy(g - 1).start()

    for g in range(4):
        k_step(g, 0, "first")

        def middle(k, _, g=g):
            k_step(g, k, "middle")
            return 0
        lax.fori_loop(1, NK - 1, middle, 0)
        k_step(g, NK - 1, "last")
        if g == 1:
            build_combine()

    def part_at(c, where, which):
        width = CHUNKS[c][1]
        return acc.at[pl.ds(pl.multiple_of(((c % 2 * 2 + where) * 2 + which) * TOK, TOK), TOK), pl.ds(0, width)]

    def cols_of(c):
        return pl.ds(CHUNKS[c][0], CHUNKS[c][1])

    def s_copy(c, i):
        return pltpu.make_async_remote_copy(
            src_ref=part_at(c, i, 1 - core), dst_ref=sib.at[i, :, cols_of(c)],
            send_sem=s_send.at[c, i], recv_sem=s_recv.at[c, i], device_id={"ep": sibling}, device_id_type=MESH)

    def r_copy(c):
        return pltpu.make_async_remote_copy(
            src_ref=sib.at[0, :, cols_of(c)], dst_ref=rem.at[:, cols_of(c)],
            send_sem=r_send.at[c], recv_sem=r_recv.at[c], device_id={"ep": partner}, device_id_type=MESH)

    def relay(c):
        cols = cols_of(c)
        s_copy(c, 0).wait_recv()
        sib[0, :, cols] = sib[0, :, cols] + part_at(c, 0, core)[...]
        r_copy(c).start()
        s_copy(c, 1).wait_recv()
        sib[1, :, cols] = sib[1, :, cols] + part_at(c, 1, core)[...]

    def combine(c):
        width = CHUNKS[c][1]
        if c >= 2:
            s_copy(c - 2, 0).wait_send()
            s_copy(c - 2, 1).wait_send()
        for i in range(2):
            ch = (1 - chip) if i == 0 else chip
            for w in range(2):
                d = ch * 2 + w
                tot = jnp.dot(cmb[d, 0], yb[d, :, 0:width], preferred_element_type=f32)
                for q in range(1, 3):
                    tot = tot + jnp.dot(cmb[d, q], yb[d, :, 0:width], preferred_element_type=f32)
                part_at(c, i, w)[...] = tot
            s_copy(c, i).start()

    for c in range(NC):
        width = CHUNKS[c][1]

        def trip(q, _, c=c, width=width):
            s0 = P1 + c * (NE // 2) + 2 * q
            if c == 0:
                @pl.when(q == NE // 4 - 1)
                def _():
                    for i in range(2):
                        a_copy(i).wait_recv()
            ys = []
            for i in range(4):
                slot = slot_of(s0, i)
                pltpu.make_async_copy(wd_hbm.at[0, :, pl.ds(0, width)], ring.at[slot, :, pl.ds(0, width)],
                                      ring_sem.at[slot]).wait()
            for i in range(4):
                ys.append(jnp.dot(act[4 * q + i], ring[slot_of(s0, i), :, 0:width], preferred_element_type=f32))
            for ch in range(2):
                r0, r1 = ch * PROW, (ch + 1) * PROW
                for w in range(2):
                    rows = [jnp.where(half[:, 0:width], ys[2 * jj + w][r0:r1], ys[2 * jj + 1 - w][r0:r1])
                            for jj in range(2)]
                    yb[2 * ch + w, pl.ds(pl.multiple_of(q * EROW, EROW), EROW), 0:width] = jnp.concatenate(
                        rows, axis=0).astype(bf16)
            low = P1 + c * (NE // 2) + AHEAD
            for i in range(2):
                fill(s0 + i + AHEAD, low + i, low + i + 6)

            if c > 0:
                @pl.when(q == 0)
                def _():
                    relay(c - 1)
            return 0

        lax.fori_loop(0, NE // 4, trip, 0)
        combine(c)
    relay(NC - 1)

    outs = []
    for c in range(NC):
        cols = cols_of(c)
        r_copy(c).wait_recv()
        xv[:, cols] = (xv[:, cols].astype(f32) + (sib[1, :, cols] + rem[:, cols])).astype(bf16)
        outs.append(pltpu.make_async_copy(xv.at[:, cols], out_hbm.at[:, cols], out_sem.at[c]))
        outs[-1].start()

    for k in range(NK):
        own_to_sibling(k).wait_send()
        own_to_partner(k).wait_send()
        hand_on(k).wait_send()
        for i in range(2):
            x_copy(k, i).wait_send()
    for i in range(2):
        a_copy(i).wait_send()
    for idx in range(3):
        pos_copy(idx).wait_send()
        gate_copy(idx).wait_send()
    for c in range(NC):
        r_copy(c).wait_send()
    for c in range(NC - 2, NC):
        for i in range(2):
            s_copy(c, i).wait_send()
    for o in outs:
        o.wait()


def solution(mesh):
    def local_block(x_in, norm_gain, w_router, expert_ids, w_gate, w_up, w_down):
        tokens, hidden = x_in.shape
        dma = pltpu.SemaphoreType.DMA
        return pl.pallas_call(
            kernel,
            out_shape=jax.ShapeDtypeStruct((tokens, hidden), bf16),
            in_specs=[pl.BlockSpec(memory_space=pl.ANY)] * 7,
            out_specs=pl.BlockSpec(memory_space=pl.ANY),
            scratch_shapes=[
                pltpu.VMEM((TOK, NK * KC), bf16),
                pltpu.VMEM((1, NK * KC), bf16),
                pltpu.VMEM((64, NK * KC), bf16),
                pltpu.VMEM((6, TOK), i32),
                pltpu.VMEM((NK, 4 * PAD, KC), bf16),
                pltpu.VMEM((4, NE, PAD), f32),
                pltpu.VMEM((4, NE, PAD), f32),
                pltpu.VMEM((4, NE, PAD), f32),
                pltpu.VMEM((4, NE, PAD), f32),
                pltpu.VMEM((4, NE // 2, GROW, PAD), bf16),
                pltpu.VMEM((4, 3, TOK, DSLOT), bf16),
                pltpu.VMEM((4 * 2 * NF * EROW, KC), f32),
                pltpu.VMEM((NE, EROW, FF), bf16),
                pltpu.VMEM((NSLOT, FF, KC), bf16),
                pltpu.VMEM((4, EROW, KC), bf16),
                pltpu.VMEM((NK, 2, 2, EROW, KC), bf16),
                pltpu.VMEM((NK, 2, EROW, KC), bf16),
                pltpu.VMEM((2, EROW, FF), bf16),
                pltpu.VMEM((4, DSLOT, KC), bf16),
                pltpu.VMEM((2, TOK, NK * KC), f32),
                pltpu.VMEM((TOK, NK * KC), f32),
                dma((4,)), dma((NC,)), dma((NSLOT,)),
                dma((NK, 3)), dma((NK, 3)),
                dma((3,)), dma((3,)), dma((3,)), dma((3,)),
                dma((NK, 2)), dma((NK, 2)), dma((2,)), dma((2,)),
                dma((NC, 2)), dma((NC, 2)), dma((NC,)), dma((NC,)),
            ],
            compiler_params=pltpu.CompilerParams(
                collective_id=0, has_side_effects=True, vmem_limit_bytes=67_043_328),
            name="moe_step",
        )(x_in, norm_gain.reshape(1, hidden), w_router.T, expert_ids.T, w_gate, w_up, w_down)

    tok_spec = P(("dp", "ep"), None)
    expert_spec = P("ep", None, None)
    return jax.shard_map(local_block, mesh=mesh, in_specs=(tok_spec, P(None), P(None, None), tok_spec, expert_spec, expert_spec, expert_spec), out_specs=tok_spec, check_vma=False)
```

```python
import jax
import jax.numpy as jnp
from jax import lax
from jax.experimental import pallas as pl
from jax.experimental.pallas import tpu as pltpu
from jax.sharding import PartitionSpec as P

EPS = 1e-6
TOK = 192
PAD = 256
CAP = 36
PROW = 2 * CAP
GROW = 80
EROW = 4 * CAP
NE = 16
DSLOT = NE // 2 * PROW
MISS = -100.0
KC = 512
NK = 5
FF = 1536
NF = 3
NSLOT = 16
AHEAD = NSLOT // 2
G0, GS, G3 = 6, 3, 2
S1 = G0 * NK
S3 = S1 + 2 * GS * NK
P1 = S3 + G3 * NK
WC = 256
NC = NK * KC // WC
P2 = NC * NE // 4
f32, bf16, i32 = jnp.float32, jnp.bfloat16, jnp.int32
MESH = pl.DeviceIdType.MESH


def kernel(x_hbm, gain_hbm, wr_hbm, ids_hbm, wg_hbm, wu_hbm, wd_hbm, out_hbm,
           xv, gv, wrv, idv, h_all, pos_own, gate_own, pos_all, gate_all, gat, cmb, acc, act, ring, xg, xy, xp, sib, rem,
           in_sem, out_sem, ring_sem, h_send, h_recv, p_send, p_recv, g_send, g_recv, x_send, x_recv, a_send, a_recv,
           s_send, s_recv, r_send, r_recv):
    me = lax.axis_index("ep")
    dp = lax.axis_index("dp")
    chip = me // 2
    core = me % 2
    sibling = chip * 2 + (1 - core)
    partner = (1 - chip) * 2 + core
    diag = (1 - chip) * 2 + (1 - core)
    peers = (partner, diag, sibling)
    twin = {"dp": 1 - dp, "ep": me}

    ins = [pltpu.make_async_copy(s, d, in_sem.at[i]) for i, (s, d) in enumerate(
        ((ids_hbm, idv), (x_hbm, xv), (gain_hbm, gv), (wr_hbm, wrv)))]
    for i in (1, 2, 0, 3):
        ins[i].start()

    def slot_of(s, i):
        return (2 * s + i) % NSLOT

    def fill_up(s, e, k):
        for m, w in enumerate((wg_hbm, wu_hbm)):
            for n in range(NF):
                pltpu.make_async_copy(
                    w.at[e, pl.ds(k * KC, KC), pl.ds(n * KC, KC)],
                    ring.at[slot_of(s, m), pl.ds(n * KC, KC)], ring_sem.at[slot_of(s, m)]).start()

    def fill_first(s):
        fill_up(s, s % G0, s // G0)

    def fill_shared(s):
        t = s - S1
        g, u = t // (GS * NK), t % (GS * NK)
        i = u % GS
        fill_up(s, 6 + 2 * g + i + i // 2 * (4 - g + 2 * dp), u // GS)

    def fill_last(s):
        fill_up(s, 10 + (s - S3) % G3, (s - S3) // G3)

    def fill_down(s):
        p = s - P1
        c, q = p // (NE // 4), p % (NE // 4)
        for i in range(4):
            slot = slot_of(s, i // 2)
            pltpu.make_async_copy(
                wd_hbm.at[4 * q + i, :, pl.ds(pl.multiple_of(c * WC, WC), WC)],
                ring.at[slot, :, pl.ds(i % 2 * WC, WC)], ring_sem.at[slot]).start()

    spans = [(0, S1, fill_first), (S1, S3, fill_shared), (S3, P1, fill_last), (P1, P1 + P2, fill_down)]

    def fill(s, low, high):
        todo = [v for v in spans if v[0] <= high and low < v[1]]
        for a, b, fn in todo:
            if a <= low and high < b:
                fn(s)
            elif b <= low or high < a:
                pass
            else:
                pl.when((s >= a) & (s < b))(lambda fn=fn: fn(s))

    def wait_up(slot):
        pltpu.make_async_copy(wd_hbm.at[0, :, pl.ds(0, KC)], ring.at[slot], ring_sem.at[slot]).wait()

    barrier = pltpu.get_barrier_semaphore()
    for d in peers:
        pl.semaphore_signal(barrier, inc=1, device_id={"ep": d}, device_id_type=MESH)
    pl.semaphore_signal(barrier, inc=1, device_id=twin, device_id_type=MESH)

    for d in range(4):
        h_all[:, d * PAD + TOK:(d + 1) * PAD, :] = jnp.zeros((NK, PAD - TOK, KC), bf16)
    for d in range(4):
        pos_own[d] = jnp.full((NE, PAD), MISS, f32)
        gate_own[d] = jnp.zeros((NE, PAD), f32)

    for c in ins[1:3]:
        c.wait()
    for s in range(AHEAD):
        fill(s, s, s)
    my_rows = pl.ds(pl.multiple_of(me * PAD, PAD), TOK)
    ssq = jnp.zeros((TOK, 1), f32)
    for k in range(NK):
        xc = xv[:, k * KC:(k + 1) * KC].astype(f32)
        ssq = ssq + jnp.sum(xc * xc, axis=1, keepdims=True)
    gains = gv[...].astype(f32)
    inv = lax.rsqrt(ssq * (1.0 / (NK * KC)) + EPS)
    for k in range(NK):
        xc = xv[:, k * KC:(k + 1) * KC].astype(f32)
        gain = jnp.concatenate([gains[4 * k + i:4 * k + i + 1, :] for i in range(4)], axis=1)
        h_all[k, my_rows, :] = (xc * inv * gain).astype(bf16)

    pl.semaphore_wait(barrier, 4)

    def small_copy(own, everyone, ss, rs, idx):
        return pltpu.make_async_remote_copy(
            src_ref=own.at[peers[idx]], dst_ref=everyone.at[me], send_sem=ss.at[idx], recv_sem=rs.at[idx],
            device_id={"ep": peers[idx]}, device_id_type=MESH)

    def pos_copy(idx):
        return small_copy(pos_own, pos_all, p_send, p_recv, idx)

    def gate_copy(idx):
        return small_copy(gate_own, gate_all, g_send, g_recv, idx)

    def h_copy(k, owner, target, ss):
        rows = pl.ds(pl.multiple_of(owner * PAD, PAD), TOK)
        return pltpu.make_async_remote_copy(
            src_ref=h_all.at[k, rows], dst_ref=h_all.at[k, rows], send_sem=h_send.at[k, ss], recv_sem=h_recv.at[k, ss],
            device_id={"ep": target}, device_id_type=MESH)

    def own_to_sibling(k):
        return h_copy(k, me, sibling, 0)

    def own_to_partner(k):
        return h_copy(k, me, partner, 1)

    def hand_on(k):
        return h_copy(k, partner, sibling, 2)

    def x_copy(k, i):
        return pltpu.make_async_remote_copy(
            src_ref=xy.at[(k * 2 + 1 - dp) * 2 + i], dst_ref=xp.at[k, i], send_sem=x_send.at[k, i], recv_sem=x_recv.at[k, i],
            device_id=twin, device_id_type=MESH)

    def a_copy(i, n):
        return pltpu.make_async_remote_copy(
            src_ref=xy.at[(n * 2 + dp) * 2 + i], dst_ref=act.at[12 + 2 * dp + i, :, pl.ds(n * KC, KC)],
            send_sem=a_send.at[i, n], recv_sem=a_recv.at[i, n], device_id=twin, device_id_type=MESH)

    own_to_partner(0).start()
    own_to_sibling(0).start()
    ins[0].wait()
    e_iota = lax.broadcasted_iota(i32, (64, TOK), 0)
    hit = jnp.zeros((64, TOK), f32)
    for j in range(6):
        hit = hit + jnp.where(idv[j:j + 1, :] == e_iota, 1.0, 0.0)
    upper = (lax.broadcasted_iota(i32, (TOK, TOK), 0) < lax.broadcasted_iota(i32, (TOK, TOK), 1)).astype(f32).astype(bf16)
    before = jnp.dot(hit.astype(bf16), upper, preferred_element_type=f32)
    pos = jnp.where(hit > 0.5, before, MISS)
    for d in range(4):
        pos_own[d, :, 0:TOK] = pos[d * NE:(d + 1) * NE]

    for idx in range(3):
        pos_copy(idx).start()
    for k in range(1, NK):
        own_to_partner(k).start()
        own_to_sibling(k).start()

    ins[3].wait()
    logits = jnp.zeros((64, TOK), f32)
    for k in range(NK):
        logits = logits + lax.dot_general(
            wrv[:, k * KC:(k + 1) * KC], h_all[k, my_rows, :], (((1,), (1,)), ((), ())), preferred_element_type=f32)
    ex = jnp.exp(logits - jnp.max(logits, axis=0, keepdims=True))
    prob = ex / jnp.sum(ex, axis=0, keepdims=True)
    picked = prob * hit
    gates = picked / jnp.sum(picked, axis=0, keepdims=True)
    for d in range(4):
        gate_own[d, :, 0:TOK] = gates[d * NE:(d + 1) * NE]
    for idx in range(3):
        gate_copy(idx).start()
    pos_all[me] = pos_own[me]
    gate_all[me] = gate_own[me]

    own_to_partner(0).wait_recv()
    hand_on(0).start()

    for idx in range(3):
        pos_copy(idx).wait_recv()

    ri = lax.broadcasted_iota(i32, (GROW, PAD), 0)
    r_iota = ri.astype(f32)
    low = ri < CAP
    for d in range(4):
        for j in range(NE // 2):
            ea, eb = 2 * j + d % 2, 2 * j + 1 - d % 2
            want = jnp.where(low, pos_all[d, ea:ea + 1, :], pos_all[d, eb:eb + 1, :] + CAP)
            gat[d, j] = jnp.where(r_iota == want, 1.0, 0.0).astype(bf16)

    def build_combine():
        for idx in range(3):
            gate_copy(idx).wait_recv()
        le = lax.broadcasted_iota(i32, (NE, DSLOT), 1)
        ee = lax.broadcasted_iota(i32, (NE, DSLOT), 0)
        lane = lax.broadcasted_iota(i32, (TOK, DSLOT), 1) % PROW
        slot_r = jnp.where(lane < CAP, lane, lane - CAP).astype(f32)
        for d in range(4):
            swap = jnp.where(le % PROW < CAP, d % 2, 1 - d % 2)
            expand = (le // PROW * 2 + swap == ee).astype(f32).astype(bf16)
            ptok = jnp.transpose(pos_all[d])[:TOK]
            wtok = jnp.transpose(gate_all[d])[:TOK]
            pexp = jnp.dot(ptok.astype(bf16), expand, preferred_element_type=f32)
            sel = pexp == slot_r
            rest = wtok
            for i in range(3):
                part = rest.astype(bf16)
                rest = rest - part.astype(f32)
                wexp = jnp.dot(part, expand, preferred_element_type=f32)
                cmb[d, i] = jnp.where(sel, wexp, 0.0).astype(bf16)

    half = lax.broadcasted_iota(i32, (PROW, KC), 0) < CAP

    def gather(k, pair, n_pair, store):
        outs = [jnp.dot(gat[d, pl.ds(pair, n_pair)].reshape(n_pair * GROW, PAD),
                        h_all[k, d * PAD:(d + 1) * PAD, :], preferred_element_type=f32) for d in range(4)]
        for jj in range(n_pair):
            o = [v[jj * GROW:jj * GROW + PROW] for v in outs]
            store(jj, 0, jnp.concatenate(
                [jnp.where(half, o[0], o[1]), jnp.where(half, o[2], o[3])], axis=0).astype(bf16))
            store(jj, 1, jnp.concatenate(
                [jnp.where(half, o[1], o[0]), jnp.where(half, o[3], o[2])], axis=0).astype(bf16))

    def k_step(s0, k, mode, experts, pair, n_pair, low, high, blocks, shared=None):
        first = shared is None and n_pair == 3
        if first:
            own_to_sibling(k).wait_recv()
            hand_on(k).wait_recv()
        if shared is not None:
            x_copy(k, shared).wait_recv()

            @pl.when(shared == 0)
            def _():
                x_copy(k, 1).start()

        def put(jj, i, v):
            xg[2 * jj + i] = v
        gather(k, pair, n_pair, put)
        if first:
            def put_shared(jj, i, v):
                xy[(k * 2 + jj) * 2 + i] = v
            gather(k, 6, 2, put_shared)
        if first:
            x_copy(k, 0).start()

        for b, block in enumerate(blocks):
            for i in block:
                for m in range(2):
                    wait_up(slot_of(s0 + i, m))
            for i in block:
                two = shared is not None and i == len(experts) - 1
                lhs = jnp.concatenate([xy[(k * 2 + dp) * 2 + shared], xp[k, shared]], axis=0) if two else xg[i]
                rows = 2 * EROW if two else EROW
                for n in range(NF):
                    val = []
                    for m in range(2):
                        r = jnp.dot(lhs, ring[slot_of(s0 + i, m), n * KC:(n + 1) * KC, :], preferred_element_type=f32)
                        at = i * 2 * NF * EROW + (m * NF + n) * rows
                        if mode == "first":
                            acc[at:at + rows, :] = r
                        elif mode == "middle":
                            acc[at:at + rows, :] = acc[at:at + rows, :] + r
                        else:
                            val.append(acc[at:at + rows, :] + r)
                    if mode == "last":
                        a = (jax.nn.silu(val[0]) * val[1]).astype(bf16)
                        cols = slice(n * KC, (n + 1) * KC)
                        act[experts[i], :, cols] = a[:EROW]
                        if two:
                            xy[(n * 2 + dp) * 2 + shared] = a[EROW:]
                            a_copy(shared, n).start()
            for i in block:
                fill(s0 + i + AHEAD, low + i + AHEAD, high + i + AHEAD)
            if first and b == 0:
                if not isinstance(k, int) or k < NK - 1:
                    own_to_partner(k + 1).wait_recv()
                    hand_on(k + 1).start()

    def k_loop(base, per, low, high, **kw):
        k_step(base, 0, "first", low=low, high=high, **kw)

        def middle(k, _):
            k_step(base + k * per, k, "middle", low=low + per, high=high + 3 * per, **kw)
            return 0
        lax.fori_loop(1, NK - 1, middle, 0)
        k_step(base + (NK - 1) * per, NK - 1, "last", low=low + (NK - 1) * per, high=high + (NK - 1) * per, **kw)

    k_loop(0, G0, 0, 0, experts=tuple(range(G0)), pair=0, n_pair=3, blocks=((0, 1), (2, 3), (4, 5)))

    def shared_group(g, _):
        k_loop(S1 + g * (GS * NK), GS, S1, S1 + GS * NK, experts=(6 + 2 * g, 7 + 2 * g, 12 + 2 * dp + g),
               pair=3 + g, n_pair=1, blocks=((0, 1, 2),), shared=g)
        return 0
    lax.fori_loop(0, 2, shared_group, 0)
    build_combine()
    k_loop(S3, G3, S3, S3, experts=(10, 11), pair=5, n_pair=1, blocks=((0, 1),))
    for k in range(NK):
        for i in range(2):
            x_copy(k, i).wait_send()
    for i in range(2):
        for n in range(NF):
            a_copy(i, n).wait_send()

    def part_rows(c, where, which):
        return pl.ds(pl.multiple_of(((c % 2 * 2 + where) * 2 + which) * TOK, TOK), TOK)

    def cols_of(c):
        return pl.ds(c * WC, WC) if isinstance(c, int) else pl.ds(pl.multiple_of(c * WC, WC), WC)

    def s_copy(c, i):
        return pltpu.make_async_remote_copy(
            src_ref=acc.at[part_rows(c, i, 1 - core), pl.ds(0, WC)], dst_ref=sib.at[i, :, cols_of(c)],
            send_sem=s_send.at[c, i], recv_sem=s_recv.at[c, i], device_id={"ep": sibling}, device_id_type=MESH)

    def r_copy(c):
        return pltpu.make_async_remote_copy(
            src_ref=sib.at[0, :, cols_of(c)], dst_ref=rem.at[:, cols_of(c)],
            send_sem=r_send.at[c], recv_sem=r_recv.at[c], device_id={"ep": partner}, device_id_type=MESH)

    def relay(c):
        cols = cols_of(c)
        s_copy(c, 0).wait_recv()
        sib[0, :, cols] = sib[0, :, cols] + acc[part_rows(c, 0, core), 0:WC]
        r_copy(c).start()
        s_copy(c, 1).wait_recv()
        sib[1, :, cols] = sib[1, :, cols] + acc[part_rows(c, 1, core), 0:WC]

    def combine(c):
        @pl.when(c >= 2)
        def _():
            s_copy(c - 2, 0).wait_send()
            s_copy(c - 2, 1).wait_send()
        for i in range(2):
            ch = (1 - chip) if i == 0 else chip
            for w in range(2):
                d = ch * 2 + w
                rows = xy[pl.ds(d * (NE // 4), NE // 4), :, 0:WC].reshape(DSLOT, WC)
                tot = jnp.dot(cmb[d, 0], rows, preferred_element_type=f32)
                for q in range(1, 3):
                    tot = tot + jnp.dot(cmb[d, q], rows, preferred_element_type=f32)
                acc[part_rows(c, i, w), 0:WC] = tot
            s_copy(c, i).start()

    narrow = half[:, 0:WC]

    def trip(t, _):
        c, r = t // 2, t % 2
        s0 = P1 + 2 * t
        @pl.when(t == 1)
        def _():
            for i in range(2):
                for n in range(NF):
                    a_copy(i, n).wait_recv()
        for i in range(4):
            wait_up(slot_of(s0, i))
        for v in range(2):
            q = 2 * r + v
            ys = [jnp.dot(act[4 * q + i], ring[slot_of(s0 + v, i // 2), :, i % 2 * WC:(i % 2 + 1) * WC],
                          preferred_element_type=f32) for i in range(4)]
            for ch in range(2):
                r0, r1 = ch * PROW, (ch + 1) * PROW
                for w in range(2):
                    rows = [jnp.where(narrow, ys[2 * jj + w][r0:r1], ys[2 * jj + 1 - w][r0:r1]) for jj in range(2)]
                    xy[(2 * ch + w) * (NE // 4) + q, :, 0:WC] = jnp.concatenate(rows, axis=0).astype(bf16)

        @pl.when(t < P2 // 2 - AHEAD // 2)
        def _():
            for i in range(2):
                fill_down(s0 + i + AHEAD)

        @pl.when((r == 0) & (c > 1))
        def _():
            relay(c - 1)

        @pl.when(r == 1)
        def _():
            combine(c)

        @pl.when(t == 1)
        def _():
            relay(0)
        return 0

    lax.fori_loop(0, P2 // 2, trip, 0)
    relay(NC - 1)

    outs = []
    for c in range(NC):
        cols = cols_of(c)
        r_copy(c).wait_recv()
        xv[:, cols] = (xv[:, cols].astype(f32) + (sib[1, :, cols] + rem[:, cols])).astype(bf16)
        outs.append(pltpu.make_async_copy(xv.at[:, cols], out_hbm.at[:, cols], out_sem.at[c]))
        outs[-1].start()

    for k in range(NK):
        own_to_sibling(k).wait_send()
        own_to_partner(k).wait_send()
        hand_on(k).wait_send()
    for idx in range(3):
        pos_copy(idx).wait_send()
        gate_copy(idx).wait_send()
    for c in range(NC):
        r_copy(c).wait_send()
    for c in range(NC - 2, NC):
        for i in range(2):
            s_copy(c, i).wait_send()
    for o in outs:
        o.wait()


def solution(mesh):
    def local_block(x_in, norm_gain, w_router, expert_ids, w_gate, w_up, w_down):
        tokens, hidden = x_in.shape
        dma = pltpu.SemaphoreType.DMA
        return pl.pallas_call(
            kernel,
            out_shape=jax.ShapeDtypeStruct((tokens, hidden), bf16),
            in_specs=[pl.BlockSpec(memory_space=pl.ANY)] * 7,
            out_specs=pl.BlockSpec(memory_space=pl.ANY),
            scratch_shapes=[
                pltpu.VMEM((TOK, NK * KC), bf16),
                pltpu.VMEM((NK * KC // 128, 128), bf16),
                pltpu.VMEM((64, NK * KC), bf16),
                pltpu.VMEM((6, TOK), i32),
                pltpu.VMEM((NK, 4 * PAD, KC), bf16),
                pltpu.VMEM((4, NE, PAD), f32),
                pltpu.VMEM((4, NE, PAD), f32),
                pltpu.VMEM((4, NE, PAD), f32),
                pltpu.VMEM((4, NE, PAD), f32),
                pltpu.VMEM((4, NE // 2, GROW, PAD), bf16),
                pltpu.VMEM((4, 3, TOK, DSLOT), bf16),
                pltpu.VMEM((G0 * 2 * NF * EROW, KC), f32),
                pltpu.VMEM((NE, EROW, FF), bf16),
                pltpu.VMEM((NSLOT, FF, KC), bf16),
                pltpu.VMEM((G0, EROW, KC), bf16),
                pltpu.VMEM((NK * 4, EROW, KC), bf16),
                pltpu.VMEM((NK, 2, EROW, KC), bf16),
                pltpu.VMEM((2, TOK, NK * KC), f32),
                pltpu.VMEM((TOK, NK * KC), f32),
                dma((4,)), dma((NC,)), dma((NSLOT,)),
                dma((NK, 3)), dma((NK, 3)),
                dma((3,)), dma((3,)), dma((3,)), dma((3,)),
                dma((NK, 2)), dma((NK, 2)), dma((2, NF)), dma((2, NF)),
                dma((NC, 2)), dma((NC, 2)), dma((NC,)), dma((NC,)),
            ],
            compiler_params=pltpu.CompilerParams(
                collective_id=0, has_side_effects=True, vmem_limit_bytes=67_043_328),
            name="moe_step",
        )(x_in, norm_gain.reshape(hidden // 128, 128), w_router.T, expert_ids.T, w_gate, w_up, w_down)

    tok_spec = P(("dp", "ep"), None)
    expert_spec = P("ep", None, None)
    return jax.shard_map(local_block, mesh=mesh, in_specs=(tok_spec, P(None), P(None, None), tok_spec, expert_spec, expert_spec, expert_spec), out_specs=tok_spec, check_vma=False)
```

```python
import jax
import jax.numpy as jnp
from jax import lax
from jax.experimental import pallas as pl
from jax.experimental.pallas import tpu as pltpu
from jax.sharding import PartitionSpec as P

EPS = 1e-6
TOK = 192
PAD = 256
CAP = 36
PROW = 2 * CAP
GROW = 80
EROW = 4 * CAP
NE = 16
DSLOT = NE // 2 * PROW
MISS = -100.0
KC = 512
NK = 5
FF = 1536
NF = 3
NSLOT = 16
AHEAD = NSLOT // 2
G0 = 6
S1 = G0 * NK
S3 = S1 + 36
P1 = S3 + 12
KB = 2 * KC
WC = 256
NC = NK * KC // WC
P2 = NC * NE // 4
f32, bf16, i32 = jnp.float32, jnp.bfloat16, jnp.int32
MESH = pl.DeviceIdType.MESH


def kernel(x_hbm, gain_hbm, wr_hbm, ids_hbm, wg_hbm, wu_hbm, wd_hbm, xv,
           gv, idv, h_all, pos_own, gate_own, pos_all, gate_all, gat, cmb, acc, act, ring, xg, xy, xp, sib, rem,
           in_sem, ring_sem, h_send, h_recv, p_send, p_recv, g_send, g_recv, x_send, x_recv, a_send, a_recv,
           s_send, s_recv, r_send, r_recv):
    me = lax.axis_index("ep")
    dp = lax.axis_index("dp")
    chip = me // 2
    core = me % 2
    sibling = chip * 2 + (1 - core)
    partner = (1 - chip) * 2 + core
    diag = (1 - chip) * 2 + (1 - core)
    peers = (partner, diag, sibling)
    twin = {"dp": 1 - dp, "ep": me}

    ins = [pltpu.make_async_copy(s, d, in_sem.at[i]) for i, (s, d) in enumerate(
        ((ids_hbm, idv), (x_hbm, xv), (gain_hbm, gv)))]
    ins += [pltpu.make_async_copy(wr_hbm.at[:, pl.ds(k * KC, KC)], xy.at[k, pl.ds(0, 64)], in_sem.at[3 + k])
            for k in range(NK)]
    for i in (1, 2, 0, 3, 4, 5, 6, 7):
        ins[i].start()

    def slot_of(s, i):
        return (2 * s + i) % NSLOT

    def fill_up(s, e, k):
        for m, w in enumerate((wg_hbm, wu_hbm)):
            for n in range(NF):
                pltpu.make_async_copy(
                    w.at[e, pl.ds(k * KC, KC), pl.ds(n * KC, KC)],
                    ring.at[slot_of(s, m), pl.ds(n * KC, KC)], ring_sem.at[slot_of(s, m)]).start()

    def fill_first(s):
        fill_up(s, s % G0, s // G0)

    def fill_unit(s, e, n, part):
        cols = pl.ds(pl.multiple_of(n * KC, KC), KC)
        for m, w in enumerate((wg_hbm, wu_hbm)):
            if part == 0:
                pltpu.make_async_copy(
                    w.at[e, pl.ds(0, FF), cols], ring.at[slot_of(s, m)], ring_sem.at[slot_of(s, m)]).start()
            else:
                pltpu.make_async_copy(w.at[e, pl.ds(FF, KB), cols], ring.at[slot_of(s, m), pl.ds(0, KB)],
                                      ring_sem.at[slot_of(s, m)]).start()

    def fill_shared(s, part):
        u = (s - S1) // 2
        g, i = u // 9, u // 3 % 3
        fill_unit(s, 6 + 2 * g + i + i // 2 * (4 - g + 2 * dp), u % 3, part)

    def fill_last(s, part):
        u = (s - S3) // 2
        fill_unit(s, 10 + u // 3, u % 3, part)

    def fill_down(s):
        p = s - P1
        c, q = p // (NE // 4), p % (NE // 4)
        for i in range(4):
            slot = slot_of(s, i // 2)
            pltpu.make_async_copy(
                wd_hbm.at[4 * q + i, :, pl.ds(pl.multiple_of(c * WC, WC), WC)],
                ring.at[slot, :, pl.ds(i % 2 * WC, WC)], ring_sem.at[slot]).start()

    spans = [(0, S1, lambda s, part: fill_first(s)), (S1, S3, fill_shared), (S3, P1, fill_last),
             (P1, P1 + P2, lambda s, part: fill_down(s))]

    def fill(s, low, high):
        part = low % 2
        todo = [v for v in spans if v[0] <= high and low < v[1]]
        for a, b, fn in todo:
            if a <= low and high < b:
                fn(s, part)
            elif b <= low or high < a:
                pass
            else:
                pl.when((s >= a) & (s < b))(lambda fn=fn: fn(s, part))

    def wait_up(slot):
        pltpu.make_async_copy(wd_hbm.at[0, :, pl.ds(0, KC)], ring.at[slot], ring_sem.at[slot]).wait()

    barrier = pltpu.get_barrier_semaphore()
    for d in peers:
        pl.semaphore_signal(barrier, inc=1, device_id={"ep": d}, device_id_type=MESH)
    pl.semaphore_signal(barrier, inc=1, device_id=twin, device_id_type=MESH)

    for d in range(4):
        pos_own[d] = jnp.full((NE, PAD), MISS, f32)
        gate_own[d] = jnp.zeros((NE, PAD), f32)

    for c in ins[1:3]:
        c.wait()
    for s in range(AHEAD):
        fill(s, s, s)
    my_rows = pl.ds(pl.multiple_of(me * TOK, TOK), TOK)
    ssq = jnp.zeros((TOK, 1), f32)
    for k in range(NK):
        xc = xv[:, k * KC:(k + 1) * KC].astype(f32)
        ssq = ssq + jnp.sum(xc * xc, axis=1, keepdims=True)
    gains = gv[...].astype(f32)
    inv = lax.rsqrt(ssq * (1.0 / (NK * KC)) + EPS)
    for k in range(NK):
        xc = xv[:, k * KC:(k + 1) * KC].astype(f32)
        gain = jnp.concatenate([gains[4 * k + i:4 * k + i + 1, :] for i in range(4)], axis=1)
        h_all[k, my_rows, :] = (xc * inv * gain).astype(bf16)

    pl.semaphore_wait(barrier, 4)

    def small_copy(own, everyone, ss, rs, idx):
        return pltpu.make_async_remote_copy(
            src_ref=own.at[peers[idx]], dst_ref=everyone.at[me], send_sem=ss.at[idx], recv_sem=rs.at[idx],
            device_id={"ep": peers[idx]}, device_id_type=MESH)

    def pos_copy(idx):
        return small_copy(pos_own, pos_all, p_send, p_recv, idx)

    def gate_copy(idx):
        return small_copy(gate_own, gate_all, g_send, g_recv, idx)

    def h_copy(k, owner, target, ss):
        rows = pl.ds(pl.multiple_of(owner * TOK, TOK), TOK)
        return pltpu.make_async_remote_copy(
            src_ref=h_all.at[k, rows], dst_ref=h_all.at[k, rows], send_sem=h_send.at[k, ss], recv_sem=h_recv.at[k, ss],
            device_id={"ep": target}, device_id_type=MESH)

    def own_to_sibling(k):
        return h_copy(k, me, sibling, 0)

    def own_to_partner(k):
        return h_copy(k, me, partner, 1)

    def hand_on(k):
        return h_copy(k, partner, sibling, 2)

    def x_copy(k, i):
        return pltpu.make_async_remote_copy(
            src_ref=xy.at[(k * 2 + 1 - dp) * 2 + i], dst_ref=xp.at[k, i], send_sem=x_send.at[k, i], recv_sem=x_recv.at[k, i],
            device_id=twin, device_id_type=MESH)

    def a_copy(i, n):
        return pltpu.make_async_remote_copy(
            src_ref=xy.at[(n * 2 + 1 - dp) * 2 + i], dst_ref=act.at[12 + 2 * dp + i, :, pl.ds(n * KC, KC)],
            send_sem=a_send.at[i, n], recv_sem=a_recv.at[i, n], device_id=twin, device_id_type=MESH)

    own_to_partner(0).start()
    own_to_sibling(0).start()
    ins[0].wait()
    e_iota = lax.broadcasted_iota(i32, (64, TOK), 0)
    hit = jnp.zeros((64, TOK), f32)
    for j in range(6):
        hit = hit + jnp.where(idv[j:j + 1, :] == e_iota, 1.0, 0.0)
    upper = (lax.broadcasted_iota(i32, (TOK, TOK), 0) < lax.broadcasted_iota(i32, (TOK, TOK), 1)).astype(f32).astype(bf16)
    before = jnp.dot(hit.astype(bf16), upper, preferred_element_type=f32)
    pos = jnp.where(hit > 0.5, before, MISS)
    for d in range(4):
        pos_own[d, :, 0:TOK] = pos[d * NE:(d + 1) * NE]

    for idx in range(3):
        pos_copy(idx).start()
    for k in range(1, NK):
        own_to_partner(k).start()
        own_to_sibling(k).start()

    for c in ins[3:]:
        c.wait()
    logits = jnp.zeros((64, TOK), f32)
    for k in range(NK):
        logits = logits + lax.dot_general(
            xy[k, 0:64, :], h_all[k, my_rows, :], (((1,), (1,)), ((), ())), preferred_element_type=f32)
    ex = jnp.exp(logits - jnp.max(logits, axis=0, keepdims=True))
    prob = ex / jnp.sum(ex, axis=0, keepdims=True)
    picked = prob * hit
    gates = picked / jnp.sum(picked, axis=0, keepdims=True)
    for d in range(4):
        gate_own[d, :, 0:TOK] = gates[d * NE:(d + 1) * NE]
    for idx in range(3):
        gate_copy(idx).start()
    pos_all[me] = pos_own[me]
    gate_all[me] = gate_own[me]

    own_to_partner(0).wait_recv()
    hand_on(0).start()

    for idx in range(3):
        pos_copy(idx).wait_recv()

    ri = lax.broadcasted_iota(i32, (GROW, PAD), 0)
    r_iota = ri.astype(f32)
    low = ri < CAP
    for d in range(4):
        for j in range(NE // 2):
            ea, eb = 2 * j + d % 2, 2 * j + 1 - d % 2
            want = jnp.where(low, pos_all[d, ea:ea + 1, :], pos_all[d, eb:eb + 1, :] + CAP)
            gat[d, j] = jnp.where(r_iota == want, 1.0, 0.0)[:, :TOK].astype(bf16)

    def build_combine():
        for idx in range(3):
            gate_copy(idx).wait_recv()
        le = lax.broadcasted_iota(i32, (NE, DSLOT), 1)
        ee = lax.broadcasted_iota(i32, (NE, DSLOT), 0)
        lane = lax.broadcasted_iota(i32, (TOK, DSLOT), 1) % PROW
        slot_r = jnp.where(lane < CAP, lane, lane - CAP).astype(f32)
        for d in range(4):
            swap = jnp.where(le % PROW < CAP, d % 2, 1 - d % 2)
            expand = (le // PROW * 2 + swap == ee).astype(f32).astype(bf16)
            ptok = jnp.transpose(pos_all[d])[:TOK]
            wtok = jnp.transpose(gate_all[d])[:TOK]
            pexp = jnp.dot(ptok.astype(bf16), expand, preferred_element_type=f32)
            sel = pexp == slot_r
            rest = wtok
            for i in range(3):
                part = rest.astype(bf16)
                rest = rest - part.astype(f32)
                wexp = jnp.dot(part, expand, preferred_element_type=f32)
                cmb[d, i] = jnp.where(sel, wexp, 0.0).astype(bf16)

    half = lax.broadcasted_iota(i32, (PROW, KC), 0) < CAP

    def gather(k, pair, n_pair, store):
        outs = [jnp.dot(gat[d, pl.ds(pair, n_pair)].reshape(n_pair * GROW, TOK),
                        h_all[k, d * TOK:(d + 1) * TOK, :], preferred_element_type=f32) for d in range(4)]
        for jj in range(n_pair):
            o = [v[jj * GROW:jj * GROW + PROW] for v in outs]
            store(jj, 0, jnp.concatenate(
                [jnp.where(half, o[0], o[1]), jnp.where(half, o[2], o[3])], axis=0).astype(bf16))
            store(jj, 1, jnp.concatenate(
                [jnp.where(half, o[1], o[0]), jnp.where(half, o[3], o[2])], axis=0).astype(bf16))

    def k_step(k, mode):
        s0 = k * G0
        low, high = (s0, s0) if isinstance(k, int) else (G0, 3 * G0)
        own_to_sibling(k).wait_recv()
        hand_on(k).wait_recv()
        def put(jj, i, v):
            xg[2 * jj + i] = v
        gather(k, 0, 3, put)

        def put_shared(jj, i, v):
            xy[(k * 2 + jj) * 2 + i] = v
        gather(k, 6, 2, put_shared)
        x_copy(k, 0).start()

        for b in range(G0 // 2):
            block = (2 * b, 2 * b + 1)
            for i in block:
                for m in range(2):
                    wait_up(slot_of(s0 + i, m))
            for i in block:
                for n in range(NF):
                    val = []
                    for m in range(2):
                        r = jnp.dot(xg[i], ring[slot_of(s0 + i, m), n * KC:(n + 1) * KC, :], preferred_element_type=f32)
                        at = ((i * 2 + m) * NF + n) * EROW
                        if mode == "first":
                            acc[at:at + EROW, :] = r
                        elif mode == "middle":
                            acc[at:at + EROW, :] = acc[at:at + EROW, :] + r
                        else:
                            val.append(acc[at:at + EROW, :] + r)
                    if mode == "last":
                        act[i, :, n * KC:(n + 1) * KC] = (jax.nn.silu(val[0]) * val[1]).astype(bf16)
            for i in block:
                fill(s0 + i + AHEAD, low + i + AHEAD, high + i + AHEAD)
            if b == (G0 // 2 - 1 if mode == "first" else 0):
                if not isinstance(k, int) or k < NK - 1:
                    own_to_partner(k + 1).wait_recv()
                    hand_on(k + 1).start()

    k_step(0, "first")

    def middle(k, _):
        k_step(k, "middle")
        return 0
    lax.fori_loop(1, NK - 1, middle, 0)
    k_step(NK - 1, "last")

    def gather_pair(pair):
        for k in range(NK):
            def put(jj, i, v):
                xg[NK * i + k] = v
            gather(k, pair, 1, put)

    def unit(s0, n, low, high, rows_of, store):
        for m in range(2):
            wait_up(slot_of(s0, m))
        for m in range(2):
            slot = slot_of(s0 + 1, m)
            pltpu.make_async_copy(wg_hbm.at[0, pl.ds(FF, KB), pl.ds(0, KC)], ring.at[slot, pl.ds(0, KB)],
                                  ring_sem.at[slot]).wait()
        lhs_a = jnp.concatenate([rows_of(k) for k in range(3)], axis=1)
        lhs_b = jnp.concatenate([rows_of(k) for k in range(3, NK)], axis=1)
        val = [jnp.dot(lhs_a, ring[slot_of(s0, m)], preferred_element_type=f32)
               + jnp.dot(lhs_b, ring[slot_of(s0 + 1, m), 0:KB, :], preferred_element_type=f32) for m in range(2)]
        store(n, (jax.nn.silu(val[0]) * val[1]).astype(bf16))
        for part in range(2):
            fill(s0 + part + AHEAD, low + part + AHEAD, high + part + AHEAD)

    def cols_ff(n):
        return pl.ds(pl.multiple_of(n * KC, KC), KC)

    def two_experts(base, e, low, high):
        def body(u, _):
            i, n = u // 3, u % 3

            def store(n, a):
                act[e + i, :, cols_ff(n)] = a
            unit(base + 2 * u, n, low, high, lambda k: xg[NK * i + k], store)
            return 0
        lax.fori_loop(0, 6, body, 0)

    def shared_group(g, _):
        gather_pair(3 + g)

        @pl.when(g == 0)
        def _():
            for k in range(NK):
                x_copy(k, 1).start()
        two_experts(S1 + 18 * g, 6 + 2 * g, S1, S1 + 28)
        for k in range(NK):
            x_copy(k, g).wait_recv()
        for n in range(NF):
            x_copy(n, g).wait_send()

        def body(n, _):
            def store(n, a):
                act[12 + 2 * dp + g, :, cols_ff(n)] = a[:EROW]
                xy[(n * 2 + 1 - dp) * 2 + g] = a[EROW:]
                a_copy(g, n).start()
            unit(S1 + 18 * g + 12 + 2 * n, n, S1 + 12, S1 + 34,
                 lambda k: jnp.concatenate([xy[(k * 2 + dp) * 2 + g], xp[k, g]], axis=0), store)
            return 0
        lax.fori_loop(0, NF, body, 0)
        return 0
    lax.fori_loop(0, 2, shared_group, 0)
    build_combine()
    gather_pair(5)
    two_experts(S3, 10, S3, S3 + 10)
    for k in range(NF, NK):
        for i in range(2):
            x_copy(k, i).wait_send()
    for i in range(2):
        for n in range(NF):
            a_copy(i, n).wait_send()

    def part_rows(c, where, which):
        return pl.ds(pl.multiple_of(((c % 2 * 2 + where) * 2 + which) * TOK, TOK), TOK)

    def cols_of(c):
        return pl.ds(c * WC, WC) if isinstance(c, int) else pl.ds(pl.multiple_of(c * WC, WC), WC)

    def s_copy(c, i):
        return pltpu.make_async_remote_copy(
            src_ref=acc.at[part_rows(c, i, 1 - core), pl.ds(0, WC)], dst_ref=sib.at[i, :, cols_of(c)],
            send_sem=s_send.at[c, i], recv_sem=s_recv.at[c, i], device_id={"ep": sibling}, device_id_type=MESH)

    def r_copy(c):
        return pltpu.make_async_remote_copy(
            src_ref=sib.at[0, :, cols_of(c)], dst_ref=rem.at[:, cols_of(c)],
            send_sem=r_send.at[c], recv_sem=r_recv.at[c], device_id={"ep": partner}, device_id_type=MESH)

    def relay(c):
        cols = cols_of(c)
        s_copy(c, 0).wait_recv()
        sib[0, :, cols] = sib[0, :, cols] + acc[part_rows(c, 0, core), 0:WC]
        r_copy(c).start()
        s_copy(c, 1).wait_recv()
        sib[1, :, cols] = sib[1, :, cols] + acc[part_rows(c, 1, core), 0:WC]

    def combine(c):
        @pl.when(c >= 2)
        def _():
            s_copy(c - 2, 0).wait_send()
            s_copy(c - 2, 1).wait_send()
        for i in range(2):
            ch = (1 - chip) if i == 0 else chip
            for w in range(2):
                d = ch * 2 + w
                rows = xy[pl.ds(d * (NE // 4), NE // 4), :, 0:WC].reshape(DSLOT, WC)
                tot = jnp.dot(cmb[d, 0], rows, preferred_element_type=f32)
                for q in range(1, 3):
                    tot = tot + jnp.dot(cmb[d, q], rows, preferred_element_type=f32)
                acc[part_rows(c, i, w), 0:WC] = tot
            s_copy(c, i).start()

    narrow = half[:, 0:WC]

    def trip(t, _):
        c, r = t // 2, t % 2
        s0 = P1 + 2 * t
        @pl.when(t == 1)
        def _():
            for i in range(2):
                for n in range(NF):
                    a_copy(i, n).wait_recv()
        for i in range(4):
            wait_up(slot_of(s0, i))
        for v in range(2):
            q = 2 * r + v
            ys = [jnp.dot(act[4 * q + i], ring[slot_of(s0 + v, i // 2), :, i % 2 * WC:(i % 2 + 1) * WC],
                          preferred_element_type=f32) for i in range(4)]
            for ch in range(2):
                r0, r1 = ch * PROW, (ch + 1) * PROW
                for w in range(2):
                    rows = [jnp.where(narrow, ys[2 * jj + w][r0:r1], ys[2 * jj + 1 - w][r0:r1]) for jj in range(2)]
                    xy[(2 * ch + w) * (NE // 4) + q, :, 0:WC] = jnp.concatenate(rows, axis=0).astype(bf16)

        @pl.when(t < P2 // 2 - AHEAD // 2)
        def _():
            for i in range(2):
                fill_down(s0 + i + AHEAD)

        @pl.when((r == 0) & (c > 1))
        def _():
            relay(c - 1)

        @pl.when(r == 1)
        def _():
            combine(c)

        @pl.when(t == 1)
        def _():
            relay(0)
        return 0

    lax.fori_loop(0, P2 // 2, trip, 0)
    relay(NC - 1)

    for c in range(NC):
        cols = cols_of(c)
        r_copy(c).wait_recv()
        xv[:, cols] = (xv[:, cols].astype(f32) + (sib[1, :, cols] + rem[:, cols])).astype(bf16)

    for k in range(NK):
        own_to_sibling(k).wait_send()
        own_to_partner(k).wait_send()
        hand_on(k).wait_send()
    for idx in range(3):
        pos_copy(idx).wait_send()
        gate_copy(idx).wait_send()
    for c in range(NC):
        r_copy(c).wait_send()
    for c in range(NC - 2, NC):
        for i in range(2):
            s_copy(c, i).wait_send()


def solution(mesh):
    def local_block(x_in, norm_gain, w_router, expert_ids, w_gate, w_up, w_down):
        tokens, hidden = x_in.shape
        dma = pltpu.SemaphoreType.DMA
        return pl.pallas_call(
            kernel,
            out_shape=pltpu.VMEM((tokens, hidden), bf16),
            in_specs=[pl.BlockSpec(memory_space=pl.ANY)] * 7,
            out_specs=pl.BlockSpec(memory_space=pltpu.VMEM),
            scratch_shapes=[
                pltpu.VMEM((NK * KC // 128, 128), bf16),
                pltpu.VMEM((6, TOK), i32),
                pltpu.VMEM((NK, 4 * TOK, KC), bf16),
                pltpu.VMEM((4, NE, PAD), f32),
                pltpu.VMEM((4, NE, PAD), f32),
                pltpu.VMEM((4, NE, PAD), f32),
                pltpu.VMEM((4, NE, PAD), f32),
                pltpu.VMEM((4, NE // 2, GROW, TOK), bf16),
                pltpu.VMEM((4, 3, TOK, DSLOT), bf16),
                pltpu.VMEM((G0 * 2 * NF * EROW, KC), f32),
                pltpu.VMEM((NE, EROW, FF), bf16),
                pltpu.VMEM((NSLOT, FF, KC), bf16),
                pltpu.VMEM((2 * NK, EROW, KC), bf16),
                pltpu.VMEM((NK * 4, EROW, KC), bf16),
                pltpu.VMEM((NK, 2, EROW, KC), bf16),
                pltpu.VMEM((2, TOK, NK * KC), f32),
                pltpu.VMEM((TOK, NK * KC), f32),
                dma((3 + NK,)), dma((NSLOT,)),
                dma((NK, 3)), dma((NK, 3)),
                dma((3,)), dma((3,)), dma((3,)), dma((3,)),
                dma((NK, 2)), dma((NK, 2)), dma((2, NF)), dma((2, NF)),
                dma((NC, 2)), dma((NC, 2)), dma((NC,)), dma((NC,)),
            ],
            compiler_params=pltpu.CompilerParams(
                collective_id=0, has_side_effects=True, vmem_limit_bytes=66_060_288),
            name="moe_step",
        )(x_in, norm_gain.reshape(hidden // 128, 128), w_router.T, expert_ids.T, w_gate, w_up, w_down)

    tok_spec = P(("dp", "ep"), None)
    expert_spec = P("ep", None, None)
    return jax.shard_map(local_block, mesh=mesh, in_specs=(tok_spec, P(None), P(None, None), tok_spec, expert_spec, expert_spec, expert_spec), out_specs=tok_spec, check_vma=False)
```

```python
import jax
import jax.numpy as jnp
from jax import lax
from jax.experimental import pallas as pl
from jax.experimental.pallas import tpu as pltpu
from jax.sharding import PartitionSpec as P

EPS = 1e-6
TOK = 192
PAD = 256
CAP = 36
PROW = 2 * CAP
GROW = 80
EROW = 4 * CAP
NE = 16
DSLOT = NE // 2 * PROW
MISS = -100.0
KC = 512
NK = 5
FF = 1536
NF = 3
NSLOT = 16
AHEAD = NSLOT // 2
G0 = 6
S1 = G0 * NK
S3 = S1 + 36
P1 = S3 + 12
KB = 2 * KC
WC = 256
NC = NK * KC // WC
P2 = NC * NE // 4
f32, bf16, i32 = jnp.float32, jnp.bfloat16, jnp.int32
MESH = pl.DeviceIdType.MESH


def kernel(x_hbm, gain_hbm, wr_hbm, ids_hbm, wg_hbm, wu_hbm, wd_hbm, xv,
           gv, idv, h_all, pos_own, gate_own, pos_all, gate_all, gat, cmb, acc, act, ring, xg, xy, xp, sib, rem,
           in_sem, ring_sem, h_send, h_recv, p_send, p_recv, g_send, g_recv, x_send, x_recv, a_send, a_recv,
           s_send, s_recv, r_send, r_recv):
    me = lax.axis_index("ep")
    dp = lax.axis_index("dp")
    chip = me // 2
    core = me % 2
    sibling = chip * 2 + (1 - core)
    partner = (1 - chip) * 2 + core
    diag = (1 - chip) * 2 + (1 - core)
    peers = (partner, diag, sibling)
    twin = {"dp": 1 - dp, "ep": me}

    ins = [pltpu.make_async_copy(s, d, in_sem.at[i]) for i, (s, d) in enumerate(
        ((ids_hbm, idv), (x_hbm, xv), (gain_hbm, gv)))]
    ins += [pltpu.make_async_copy(wr_hbm.at[:, pl.ds(k * KC, KC)], xy.at[k, pl.ds(0, 64)], in_sem.at[3 + k])
            for k in range(NK)]
    for i in (1, 2, 0, 3, 4, 5, 6, 7):
        ins[i].start()

    def slot_of(s, i):
        return (2 * s + i) % NSLOT

    def fill_up(s, e, k):
        for m, w in enumerate((wg_hbm, wu_hbm)):
            for n in range(NF):
                pltpu.make_async_copy(
                    w.at[e, pl.ds(k * KC, KC), pl.ds(n * KC, KC)],
                    ring.at[slot_of(s, m), pl.ds(n * KC, KC)], ring_sem.at[slot_of(s, m)]).start()

    def fill_first(s):
        fill_up(s, s % G0, s // G0)

    def fill_unit(s, e, n, part):
        cols = pl.ds(pl.multiple_of(n * KC, KC), KC)
        for m, w in enumerate((wg_hbm, wu_hbm)):
            if part == 0:
                pltpu.make_async_copy(
                    w.at[e, pl.ds(0, FF), cols], ring.at[slot_of(s, m)], ring_sem.at[slot_of(s, m)]).start()
            else:
                pltpu.make_async_copy(w.at[e, pl.ds(FF, KB), cols], ring.at[slot_of(s, m), pl.ds(0, KB)],
                                      ring_sem.at[slot_of(s, m)]).start()

    def fill_shared(s, part):
        u = (s - S1) // 2
        g, i = u // 9, u // 3 % 3
        fill_unit(s, 6 + 2 * g + i + i // 2 * (4 - g + 2 * dp), u % 3, part)

    def fill_last(s, part):
        u = (s - S3) // 2
        fill_unit(s, 10 + u // 3, u % 3, part)

    def fill_down(s):
        p = s - P1
        c, q = p // (NE // 4), p % (NE // 4)
        for i in range(4):
            slot = slot_of(s, i // 2)
            pltpu.make_async_copy(
                wd_hbm.at[4 * q + i, :, pl.ds(pl.multiple_of(c * WC, WC), WC)],
                ring.at[slot, :, pl.ds(i % 2 * WC, WC)], ring_sem.at[slot]).start()

    spans = [(0, S1, lambda s, part: fill_first(s)), (S1, S3, fill_shared), (S3, P1, fill_last),
             (P1, P1 + P2, lambda s, part: fill_down(s))]

    def fill(s, low, high):
        part = low % 2
        todo = [v for v in spans if v[0] <= high and low < v[1]]
        for a, b, fn in todo:
            if a <= low and high < b:
                fn(s, part)
            elif b <= low or high < a:
                pass
            else:
                pl.when((s >= a) & (s < b))(lambda fn=fn: fn(s, part))

    def wait_up(slot):
        pltpu.make_async_copy(wd_hbm.at[0, :, pl.ds(0, KC)], ring.at[slot], ring_sem.at[slot]).wait()

    barrier = pltpu.get_barrier_semaphore()
    for d in peers:
        pl.semaphore_signal(barrier, inc=1, device_id={"ep": d}, device_id_type=MESH)
    pl.semaphore_signal(barrier, inc=1, device_id=twin, device_id_type=MESH)

    for d in range(4):
        pos_own[d] = jnp.full((NE, PAD), MISS, f32)
        gate_own[d] = jnp.zeros((NE, PAD), f32)

    for c in ins[1:3]:
        c.wait()
    for s in range(AHEAD):
        fill(s, s, s)
    my_rows = pl.ds(pl.multiple_of(me * TOK, TOK), TOK)
    ssq = jnp.zeros((TOK, 1), f32)
    for k in range(NK):
        xc = xv[:, k * KC:(k + 1) * KC].astype(f32)
        ssq = ssq + jnp.sum(xc * xc, axis=1, keepdims=True)
    gains = gv[...].astype(f32)
    inv = lax.rsqrt(ssq * (1.0 / (NK * KC)) + EPS)
    for k in range(NK):
        xc = xv[:, k * KC:(k + 1) * KC].astype(f32)
        gain = jnp.concatenate([gains[4 * k + i:4 * k + i + 1, :] for i in range(4)], axis=1)
        h_all[k, my_rows, :] = (xc * inv * gain).astype(bf16)

    pl.semaphore_wait(barrier, 4)

    def small_copy(own, everyone, ss, rs, idx):
        return pltpu.make_async_remote_copy(
            src_ref=own.at[peers[idx]], dst_ref=everyone.at[me], send_sem=ss.at[idx], recv_sem=rs.at[idx],
            device_id={"ep": peers[idx]}, device_id_type=MESH)

    def pos_copy(idx):
        return small_copy(pos_own, pos_all, p_send, p_recv, idx)

    def gate_copy(idx):
        return small_copy(gate_own, gate_all, g_send, g_recv, idx)

    def h_copy(k, owner, target, ss):
        rows = pl.ds(pl.multiple_of(owner * TOK, TOK), TOK)
        return pltpu.make_async_remote_copy(
            src_ref=h_all.at[k, rows], dst_ref=h_all.at[k, rows], send_sem=h_send.at[k, ss], recv_sem=h_recv.at[k, ss],
            device_id={"ep": target}, device_id_type=MESH)

    def own_to_sibling(k):
        return h_copy(k, me, sibling, 0)

    def own_to_partner(k):
        return h_copy(k, me, partner, 1)

    def hand_on(k):
        return h_copy(k, partner, sibling, 2)

    def x_copy(k, i):
        return pltpu.make_async_remote_copy(
            src_ref=xy.at[(k * 2 + 1 - dp) * 2 + i], dst_ref=xp.at[k, i], send_sem=x_send.at[k, i], recv_sem=x_recv.at[k, i],
            device_id=twin, device_id_type=MESH)

    def a_copy(i, n):
        return pltpu.make_async_remote_copy(
            src_ref=xy.at[(n * 2 + 1 - dp) * 2 + i], dst_ref=act.at[12 + 2 * dp + i, :, pl.ds(n * KC, KC)],
            send_sem=a_send.at[i, n], recv_sem=a_recv.at[i, n], device_id=twin, device_id_type=MESH)

    own_to_partner(0).start()
    own_to_sibling(0).start()
    ins[0].wait()
    e_iota = lax.broadcasted_iota(i32, (64, TOK), 0)
    hit = jnp.zeros((64, TOK), f32)
    for j in range(6):
        hit = hit + jnp.where(idv[j:j + 1, :] == e_iota, 1.0, 0.0)
    upper = (lax.broadcasted_iota(i32, (TOK, TOK), 0) < lax.broadcasted_iota(i32, (TOK, TOK), 1)).astype(f32).astype(bf16)
    before = jnp.dot(hit.astype(bf16), upper, preferred_element_type=f32)
    pos = jnp.where(hit > 0.5, before, MISS)
    for d in range(4):
        pos_own[d, :, 0:TOK] = pos[d * NE:(d + 1) * NE]

    for idx in range(3):
        pos_copy(idx).start()
    for k in range(1, NK):
        own_to_partner(k).start()
        own_to_sibling(k).start()

    for c in ins[3:]:
        c.wait()
    logits = jnp.zeros((64, TOK), f32)
    for k in range(NK):
        logits = logits + lax.dot_general(
            xy[k, 0:64, :], h_all[k, my_rows, :], (((1,), (1,)), ((), ())), preferred_element_type=f32)
    ex = jnp.exp(logits - jnp.max(logits, axis=0, keepdims=True))
    prob = ex / jnp.sum(ex, axis=0, keepdims=True)
    picked = prob * hit
    gates = picked / jnp.sum(picked, axis=0, keepdims=True)
    for d in range(4):
        gate_own[d, :, 0:TOK] = gates[d * NE:(d + 1) * NE]
    for idx in range(3):
        gate_copy(idx).start()
    pos_all[me] = pos_own[me]
    gate_all[me] = gate_own[me]

    own_to_partner(0).wait_recv()
    hand_on(0).start()

    for idx in range(3):
        pos_copy(idx).wait_recv()

    ri = lax.broadcasted_iota(i32, (GROW, PAD), 0)
    r_iota = ri.astype(f32)
    low = ri < CAP
    for d in range(4):
        for j in range(NE // 2):
            ea, eb = 2 * j + d % 2, 2 * j + 1 - d % 2
            want = jnp.where(low, pos_all[d, ea:ea + 1, :], pos_all[d, eb:eb + 1, :] + CAP)
            gat[d, j] = jnp.where(r_iota == want, 1.0, 0.0)[:, :TOK].astype(bf16)

    def build_combine():
        for idx in range(3):
            gate_copy(idx).wait_recv()
        le = lax.broadcasted_iota(i32, (NE, DSLOT), 1)
        ee = lax.broadcasted_iota(i32, (NE, DSLOT), 0)
        lane = lax.broadcasted_iota(i32, (48, DSLOT), 1) % PROW
        slot_r = jnp.where(lane < CAP, lane, lane - CAP).astype(f32)
        for d in range(4):
            swap = jnp.where(le % PROW < CAP, d % 2, 1 - d % 2)
            expand = (le // PROW * 2 + swap == ee).astype(f32).astype(bf16)
            ptok = jnp.transpose(pos_all[d])[:TOK]
            wtok = jnp.transpose(gate_all[d])[:TOK]
            for t in range(0, TOK, 48):
                pexp = jnp.dot(ptok[t:t + 48].astype(bf16), expand, preferred_element_type=f32)
                sel = pexp == slot_r
                rest = wtok[t:t + 48]
                parts = []
                for i in range(3):
                    part = rest.astype(bf16)
                    rest = rest - part.astype(f32)
                    parts.append(jnp.where(sel, jnp.dot(part, expand, preferred_element_type=f32), 0.0))
                cmb[d, t:t + 48, :] = jnp.concatenate(parts, axis=1).astype(bf16)

    half = lax.broadcasted_iota(i32, (PROW, KC), 0) < CAP

    def gather(k, pair, n_pair, store):
        outs = [jnp.dot(gat[d, pl.ds(pair, n_pair)].reshape(n_pair * GROW, TOK),
                        h_all[k, d * TOK:(d + 1) * TOK, :], preferred_element_type=f32) for d in range(4)]
        for jj in range(n_pair):
            o = [v[jj * GROW:jj * GROW + PROW] for v in outs]
            store(jj, 0, jnp.concatenate(
                [jnp.where(half, o[0], o[1]), jnp.where(half, o[2], o[3])], axis=0).astype(bf16))
            store(jj, 1, jnp.concatenate(
                [jnp.where(half, o[1], o[0]), jnp.where(half, o[3], o[2])], axis=0).astype(bf16))

    def k_step(k, mode):
        s0 = k * G0
        low, high = (s0, s0) if isinstance(k, int) else (G0, 3 * G0)
        own_to_sibling(k).wait_recv()
        hand_on(k).wait_recv()
        def put(jj, i, v):
            xg[2 * jj + i] = v
        gather(k, 0, 3, put)

        def put_shared(jj, i, v):
            xy[(k * 2 + jj) * 2 + i] = v
        gather(k, 6, 2, put_shared)
        x_copy(k, 0).start()

        for b in range(G0 // 2):
            block = (2 * b, 2 * b + 1)
            for i in block:
                for m in range(2):
                    wait_up(slot_of(s0 + i, m))
            for i in block:
                for n in range(NF):
                    val = []
                    for m in range(2):
                        r = jnp.dot(xg[i], ring[slot_of(s0 + i, m), n * KC:(n + 1) * KC, :], preferred_element_type=f32)
                        at = ((i * 2 + m) * NF + n) * EROW
                        if mode == "first":
                            acc[at:at + EROW, :] = r
                        elif mode == "middle":
                            acc[at:at + EROW, :] = acc[at:at + EROW, :] + r
                        else:
                            val.append(acc[at:at + EROW, :] + r)
                    if mode == "last":
                        act[i, :, n * KC:(n + 1) * KC] = (jax.nn.silu(val[0]) * val[1]).astype(bf16)
            for i in block:
                fill(s0 + i + AHEAD, low + i + AHEAD, high + i + AHEAD)
            if b == (G0 // 2 - 1 if mode == "first" else 0):
                if not isinstance(k, int) or k < NK - 1:
                    own_to_partner(k + 1).wait_recv()
                    hand_on(k + 1).start()

    k_step(0, "first")

    def middle(k, _):
        k_step(k, "middle")
        return 0
    lax.fori_loop(1, NK - 1, middle, 0)
    k_step(NK - 1, "last")

    def gather_pair(pair):
        for k in range(NK):
            def put(jj, i, v):
                xg[NK * i + k] = v
            gather(k, pair, 1, put)

    def unit(s0, n, low, high, rows_of, store):
        for m in range(2):
            wait_up(slot_of(s0, m))
        for m in range(2):
            slot = slot_of(s0 + 1, m)
            pltpu.make_async_copy(wg_hbm.at[0, pl.ds(FF, KB), pl.ds(0, KC)], ring.at[slot, pl.ds(0, KB)],
                                  ring_sem.at[slot]).wait()
        lhs_a = jnp.concatenate([rows_of(k) for k in range(3)], axis=1)
        lhs_b = jnp.concatenate([rows_of(k) for k in range(3, NK)], axis=1)
        val = [jnp.dot(lhs_a, ring[slot_of(s0, m)], preferred_element_type=f32)
               + jnp.dot(lhs_b, ring[slot_of(s0 + 1, m), 0:KB, :], preferred_element_type=f32) for m in range(2)]
        store(n, (jax.nn.silu(val[0]) * val[1]).astype(bf16))
        for part in range(2):
            fill(s0 + part + AHEAD, low + part + AHEAD, high + part + AHEAD)

    def cols_ff(n):
        return pl.ds(pl.multiple_of(n * KC, KC), KC)

    def two_experts(base, e, low, high):
        def body(u, _):
            i, n = u // 3, u % 3

            def store(n, a):
                act[e + i, :, cols_ff(n)] = a
            unit(base + 2 * u, n, low, high, lambda k: xg[NK * i + k], store)
            return 0
        lax.fori_loop(0, 6, body, 0)

    def shared_group(g, _):
        gather_pair(3 + g)

        @pl.when(g == 0)
        def _():
            for k in range(NK):
                x_copy(k, 1).start()
        two_experts(S1 + 18 * g, 6 + 2 * g, S1, S1 + 28)
        for k in range(NK):
            x_copy(k, g).wait_recv()
        for n in range(NF):
            x_copy(n, g).wait_send()

        def body(n, _):
            def store(n, a):
                act[12 + 2 * dp + g, :, cols_ff(n)] = a[:EROW]
                xy[(n * 2 + 1 - dp) * 2 + g] = a[EROW:]
                a_copy(g, n).start()
            unit(S1 + 18 * g + 12 + 2 * n, n, S1 + 12, S1 + 34,
                 lambda k: jnp.concatenate([xy[(k * 2 + dp) * 2 + g], xp[k, g]], axis=0), store)
            return 0
        lax.fori_loop(0, NF, body, 0)
        return 0
    lax.fori_loop(0, 2, shared_group, 0)
    build_combine()
    gather_pair(5)
    two_experts(S3, 10, S3, S3 + 10)
    for k in range(NF, NK):
        for i in range(2):
            x_copy(k, i).wait_send()
    for i in range(2):
        for n in range(NF):
            a_copy(i, n).wait_send()

    def part_rows(c, where, which):
        return pl.ds(pl.multiple_of(((c % 2 * 2 + where) * 2 + which) * TOK, TOK), TOK)

    def cols_of(c):
        return pl.ds(c * WC, WC) if isinstance(c, int) else pl.ds(pl.multiple_of(c * WC, WC), WC)

    def s_copy(c, i):
        return pltpu.make_async_remote_copy(
            src_ref=acc.at[part_rows(c, i, 1 - core), pl.ds(0, WC)], dst_ref=sib.at[i, :, cols_of(c)],
            send_sem=s_send.at[c, i], recv_sem=s_recv.at[c, i], device_id={"ep": sibling}, device_id_type=MESH)

    def r_copy(c):
        return pltpu.make_async_remote_copy(
            src_ref=sib.at[0, :, cols_of(c)], dst_ref=rem.at[:, cols_of(c)],
            send_sem=r_send.at[c], recv_sem=r_recv.at[c], device_id={"ep": partner}, device_id_type=MESH)

    def relay(c):
        cols = cols_of(c)
        s_copy(c, 0).wait_recv()
        sib[0, :, cols] = sib[0, :, cols] + acc[part_rows(c, 0, core), 0:WC]
        r_copy(c).start()

    def settle(c):
        cols = cols_of(c)
        s_copy(c, 1).wait_recv()
        sib[1, :, cols] = sib[1, :, cols] + acc[part_rows(c, 1, core), 0:WC]

    def combine(c):
        @pl.when(c >= 2)
        def _():
            s_copy(c - 2, 0).wait_send()
            s_copy(c - 2, 1).wait_send()
        for i in range(2):
            ch = (1 - chip) if i == 0 else chip
            for w in range(2):
                d = ch * 2 + w
                rows = xy[pl.ds(d * (NE // 4), NE // 4), :, 0:WC].reshape(DSLOT, WC)
                acc[part_rows(c, i, w), 0:WC] = jnp.dot(
                    cmb[d], jnp.concatenate([rows] * 3, axis=0), preferred_element_type=f32)
            s_copy(c, i).start()

    narrow = half[:, 0:WC]

    def trip(t, _):
        c, r = t // 2, t % 2
        s0 = P1 + 2 * t
        @pl.when(t == 1)
        def _():
            for i in range(2):
                for n in range(NF):
                    a_copy(i, n).wait_recv()
        for i in range(4):
            wait_up(slot_of(s0, i))
        for v in range(2):
            q = 2 * r + v
            ys = [jnp.dot(act[4 * q + i], ring[slot_of(s0 + v, i // 2), :, i % 2 * WC:(i % 2 + 1) * WC],
                          preferred_element_type=f32) for i in range(4)]
            for ch in range(2):
                r0, r1 = ch * PROW, (ch + 1) * PROW
                for w in range(2):
                    rows = [jnp.where(narrow, ys[2 * jj + w][r0:r1], ys[2 * jj + 1 - w][r0:r1]) for jj in range(2)]
                    xy[(2 * ch + w) * (NE // 4) + q, :, 0:WC] = jnp.concatenate(rows, axis=0).astype(bf16)

        @pl.when(t < P2 // 2 - AHEAD // 2)
        def _():
            for i in range(2):
                fill_down(s0 + i + AHEAD)

        @pl.when((r == 0) & (c > 0))
        def _():
            settle(c - 1)

        @pl.when(r == 1)
        def _():
            combine(c)
            relay(c)
        return 0

    lax.fori_loop(0, P2 // 2, trip, 0)
    settle(NC - 1)

    for c in range(NC):
        cols = cols_of(c)
        r_copy(c).wait_recv()
        xv[:, cols] = (xv[:, cols].astype(f32) + (sib[1, :, cols] + rem[:, cols])).astype(bf16)

    for k in range(NK):
        own_to_sibling(k).wait_send()
        own_to_partner(k).wait_send()
        hand_on(k).wait_send()
    for idx in range(3):
        pos_copy(idx).wait_send()
        gate_copy(idx).wait_send()
    for c in range(NC):
        r_copy(c).wait_send()
    for c in range(NC - 2, NC):
        for i in range(2):
            s_copy(c, i).wait_send()


def solution(mesh):
    def local_block(x_in, norm_gain, w_router, expert_ids, w_gate, w_up, w_down):
        tokens, hidden = x_in.shape
        dma = pltpu.SemaphoreType.DMA
        return pl.pallas_call(
            kernel,
            out_shape=pltpu.VMEM((tokens, hidden), bf16),
            in_specs=[pl.BlockSpec(memory_space=pl.ANY)] * 7,
            out_specs=pl.BlockSpec(memory_space=pltpu.VMEM),
            scratch_shapes=[
                pltpu.VMEM((NK * KC // 128, 128), bf16),
                pltpu.VMEM((6, TOK), i32),
                pltpu.VMEM((NK, 4 * TOK, KC), bf16),
                pltpu.VMEM((4, NE, PAD), f32),
                pltpu.VMEM((4, NE, PAD), f32),
                pltpu.VMEM((4, NE, PAD), f32),
                pltpu.VMEM((4, NE, PAD), f32),
                pltpu.VMEM((4, NE // 2, GROW, TOK), bf16),
                pltpu.VMEM((4, TOK, 3 * DSLOT), bf16),
                pltpu.VMEM((G0 * 2 * NF * EROW, KC), f32),
                pltpu.VMEM((NE, EROW, FF), bf16),
                pltpu.VMEM((NSLOT, FF, KC), bf16),
                pltpu.VMEM((2 * NK, EROW, KC), bf16),
                pltpu.VMEM((NK * 4, EROW, KC), bf16),
                pltpu.VMEM((NK, 2, EROW, KC), bf16),
                pltpu.VMEM((2, TOK, NK * KC), f32),
                pltpu.VMEM((TOK, NK * KC), f32),
                dma((3 + NK,)), dma((NSLOT,)),
                dma((NK, 3)), dma((NK, 3)),
                dma((3,)), dma((3,)), dma((3,)), dma((3,)),
                dma((NK, 2)), dma((NK, 2)), dma((2, NF)), dma((2, NF)),
                dma((NC, 2)), dma((NC, 2)), dma((NC,)), dma((NC,)),
            ],
            compiler_params=pltpu.CompilerParams(
                collective_id=0, has_side_effects=True, vmem_limit_bytes=66_060_288),
            name="moe_step",
        )(x_in, norm_gain.reshape(hidden // 128, 128), w_router.T, expert_ids.T, w_gate, w_up, w_down)

    tok_spec = P(("dp", "ep"), None)
    expert_spec = P("ep", None, None)
    return jax.shard_map(local_block, mesh=mesh, in_specs=(tok_spec, P(None), P(None, None), tok_spec, expert_spec, expert_spec, expert_spec), out_specs=tok_spec, check_vma=False)
```
